32 devices in a mesh: dp: 2 (over x), sp: 4 (over z), cp: 4 (over y, core).
Axes of the slice: x: 2, y: 2, z: 4, core: 2. Of those that a mesh axis runs over, the one named last changes fastest.
Arguments:
- hidden: bfloat16 [8192, 3072], P(('dp', 'sp', 'cp')), parts along dimension 0
- g_kv: bfloat16 [3072], replicated
- w_k: bfloat16 [3072, 3072], replicated
- w_v: bfloat16 [3072, 3072], replicated
- g_attn: bfloat16 [2, 3072], replicated
- g_mlp: bfloat16 [2, 3072], replicated
- w_q: bfloat16 [2, 3072, 3072], replicated
- w_o: bfloat16 [2, 32, 96, 3072], replicated
- w_gate: bfloat16 [2, 3072, 8192], replicated
- w_up: bfloat16 [2, 3072, 8192], replicated
- w_down: bfloat16 [2, 8192, 3072], replicated
Outputs:
- output: bfloat16 [8192, 3072], P(('dp', 'sp', 'cp')), parts along dimension 0
There are 2 independent parts. The reference program is written for one: setup_inputs(seed, part) draws one part's arguments, and reference() takes and returns one part's arrays. A program takes and returns all parts, laid end to end along the dimension named above; an argument that names none is the same for every part.
All inputs are finite; a program needn't handle non-finite values.
Results may differ from the reference program's by a relative error of at most 0.0173681.
Values are sent between devices in bfloat16 or wider.
A program may use at most 1.75 GiB of HBM per device.

```python
import jax
import jax.numpy as jnp
from jax import lax

D = 3072
HEADS = 32
KV_HEADS = 32
HEAD = 96
FF = 8192
LAYERS = 2
SEQ = 4096
QUERY_ROWS = 64
TOPICS = 8
GROUPS = HEADS // KV_HEADS


def rms_norm(values, gain_vec):
    widened = values.astype(jnp.float32)
    inv_rms = lax.rsqrt(jnp.mean(widened * widened, axis=-1, keepdims=True) + 1e-6)
    return (widened * inv_rms * gain_vec.astype(jnp.float32)).astype(jnp.bfloat16)


def setup_inputs(seed: int = 0, part: int = 0) -> dict:
    base_key = jax.random.key(seed)
    part_key = jax.random.fold_in(base_key, part)
    noise_key, topic_key = jax.random.split(part_key)
    weight_keys = jax.random.split(base_key, 10)
    noise = jax.random.normal(noise_key, (SEQ, D), jnp.float32)
    topic_rows = jax.random.normal(topic_key, (TOPICS, D), jnp.float32)
    hidden = 0.6 * noise + 0.8 * jnp.repeat(topic_rows, SEQ // TOPICS, axis=0)

    def gain_draw(key_in, shape_in):
        return jax.random.uniform(key_in, shape_in, jnp.float32, 0.5, 1.5).astype(jnp.bfloat16)

    def weight_draw(key_in, shape_in, fan_in, factor):
        return (jax.random.normal(key_in, shape_in, jnp.float32) * (factor * fan_in ** -0.5)).astype(jnp.bfloat16)

    return {
        'hidden': hidden.astype(jnp.bfloat16),
        'g_kv': gain_draw(weight_keys[0], (D,)),
        'w_k': weight_draw(weight_keys[1], (D, KV_HEADS * HEAD), D, 1.0),
        'w_v': weight_draw(weight_keys[2], (D, KV_HEADS * HEAD), D, 1.0),
        'g_attn': gain_draw(weight_keys[3], (LAYERS, D)),
        'g_mlp': gain_draw(weight_keys[4], (LAYERS, D)),
        'w_q': weight_draw(weight_keys[5], (LAYERS, D, HEADS * HEAD), D, 1.5),
        'w_o': weight_draw(weight_keys[6], (LAYERS, HEADS, HEAD, D), HEADS * HEAD, 1.0),
        'w_gate': weight_draw(weight_keys[7], (LAYERS, D, FF), D, 1.0),
        'w_up': weight_draw(weight_keys[8], (LAYERS, D, FF), D, 1.0),
        'w_down': weight_draw(weight_keys[9], (LAYERS, FF, D), FF, 1.0),
    }


def attention(query, keys, values):
    key_wide = keys.astype(jnp.float32)
    value_wide = values.astype(jnp.float32)
    key_pos = jnp.arange(SEQ)
    query_blocks = query.reshape(SEQ // QUERY_ROWS, QUERY_ROWS, GROUPS, KV_HEADS, HEAD)

    def one_block(block_in):
        q_block, block_idx = block_in
        query_pos = block_idx * QUERY_ROWS + jnp.arange(QUERY_ROWS)
        scores = jnp.einsum('trgd,sgd->trgs', q_block.astype(jnp.float32), key_wide) * (HEAD ** -0.5)
        allowed = key_pos[None, :] <= query_pos[:, None]
        scores = jnp.where(allowed[:, None, None, :], scores, -jnp.inf)
        row_max = jnp.max(scores, axis=-1, keepdims=True)
        probs = jnp.exp(scores - row_max)
        prob_sum = jnp.sum(probs, axis=-1, keepdims=True)
        probs_low = probs.astype(jnp.bfloat16).astype(jnp.float32)
        mixed = jnp.einsum('trgs,sgd->trgd', probs_low, value_wide)
        return (mixed / prob_sum).astype(jnp.bfloat16)

    outputs = lax.map(one_block, (query_blocks, jnp.arange(SEQ // QUERY_ROWS)))
    return outputs.reshape(SEQ, HEADS * HEAD)


def reference(hidden, g_kv, w_k, w_v, g_attn, g_mlp, w_q, w_o, w_gate, w_up, w_down):
    normed = rms_norm(hidden, g_kv)
    keys = jnp.dot(normed, w_k, preferred_element_type=jnp.float32).astype(jnp.bfloat16).reshape(SEQ, KV_HEADS, HEAD)
    values = jnp.dot(normed, w_v, preferred_element_type=jnp.float32).astype(jnp.bfloat16).reshape(SEQ, KV_HEADS, HEAD)

    def layer_fn(current, params):
        gain_attn, gain_mlp, wq_layer, wo_layer, gate_layer, up_layer, down_layer = params
        query = jnp.dot(rms_norm(current, gain_attn), wq_layer, preferred_element_type=jnp.float32).astype(jnp.bfloat16)
        mixed = attention(query, keys, values)
        attn_out = jnp.dot(mixed, wo_layer.reshape(HEADS * HEAD, D), preferred_element_type=jnp.float32).astype(jnp.bfloat16)
        current = (current.astype(jnp.float32) + attn_out.astype(jnp.float32)).astype(jnp.bfloat16)
        normed_mlp = rms_norm(current, gain_mlp)
        gate_out = jnp.dot(normed_mlp, gate_layer, preferred_element_type=jnp.float32).astype(jnp.bfloat16)
        up_out = jnp.dot(normed_mlp, up_layer, preferred_element_type=jnp.float32).astype(jnp.bfloat16)
        inner = (jax.nn.silu(gate_out.astype(jnp.float32)) * up_out.astype(jnp.float32)).astype(jnp.bfloat16)
        down_out = jnp.dot(inner, down_layer, preferred_element_type=jnp.float32).astype(jnp.bfloat16)
        current = (current.astype(jnp.float32) + down_out.astype(jnp.float32)).astype(jnp.bfloat16)
        return current, None

    result, unused = lax.scan(layer_fn, hidden, (g_attn, g_mlp, w_q, w_o, w_gate, w_up, w_down))
    return result
```

```python
import functools

import jax
import jax.numpy as jnp
from jax import lax
from jax.experimental import pallas as pl
from jax.experimental.pallas import tpu as pltpu
from jax.sharding import PartitionSpec as P

F32 = jnp.float32
BF16 = jnp.bfloat16
NEG_BIG = -1e30
LOOKAHEAD = 4
COLS = 512
DOWN_COLS = 256
KV_CHUNKS = 4
LOG2E = 1.4426950408889634


def rms_norm(values, gain_vec):
    widened = values.astype(F32)
    inv_rms = lax.rsqrt(jnp.mean(widened * widened, axis=-1, keepdims=True) + 1e-6)
    return (widened * inv_rms * gain_vec.astype(F32)).astype(BF16)


def kv_kernel(core_ref, x_ref, wk_ref, wv_ref, *refs):
    k_ref, v_ref = refs[-2:]
    x = x_ref[...]
    shape = k_ref.shape
    k = jnp.dot(x, wk_ref[...], preferred_element_type=F32).astype(BF16)
    k_ref[...] = k.reshape(shape)
    v = jnp.dot(x, wv_ref[...], preferred_element_type=F32).astype(BF16)
    v_ref[...] = v.reshape(shape)


def kv_project(core, x, w_k, w_v, chunk, devices, prior):
    rows, width = x.shape
    half = w_k.shape[1] // 2
    part = rows // devices
    steps = half // COLS
    out_spec = pl.BlockSpec((devices, 1, part, COLS), lambda n, c: (0, chunk, 0, n))
    w_spec = pl.BlockSpec((width, COLS), lambda n, c: (0, c[0] * steps + n))
    full = jax.ShapeDtypeStruct((devices, KV_CHUNKS, part, half), BF16)
    in_specs = [pl.BlockSpec((rows, width), lambda n, c: (0, 0)), w_spec, w_spec]
    args = [core, x, w_k, w_v]
    aliases = {}
    if prior is not None:
        in_specs += [pl.BlockSpec(memory_space=pl.ANY)] * 2
        args += list(prior)
        aliases = {4: 0, 5: 1}
    return pl.pallas_call(
        kv_kernel,
        grid_spec=pltpu.PrefetchScalarGridSpec(
            num_scalar_prefetch=1, grid=(steps,), in_specs=in_specs, out_specs=[out_spec, out_spec]
        ),
        out_shape=[full, full],
        input_output_aliases=aliases,
        cost_estimate=pl.CostEstimate(
            flops=4 * rows * width * half, bytes_accessed=2 * (rows * width + 2 * width * half + 2 * rows * half), transcendentals=0
        ),
        name="kv_project",
    )(*args)


def attention_kernel(scale, info_ref, qa_ref, qb_ref, k_ref, v_ref, oa_ref, ob_ref, q_scr, m_scr, l_scr, acc_scr):
    rows = qa_ref.shape[0]
    span = 2 * rows
    full_blocks = info_ref[1]
    a_odd = info_ref[2]
    lane = lax.broadcasted_iota(jnp.int32, (rows, 256), 1)
    window_out = []
    for window in range(2):
        offset = 128 * window
        bounds = ((0, 96), (96, 192)) if window == 0 else ((64, 160), (160, 256))
        for head in range(2):
            lo, hi = bounds[head]
            keep = (lane >= lo) & (lane < hi)
            for part in range(2):
                q_src = qa_ref if part == 0 else qb_ref
                q_win = q_src[:, offset:offset + 256]
                q_scr[2 * head + part] = jnp.where(keep, q_win, jnp.zeros_like(q_win))
        m_scr[...] = jnp.full(m_scr.shape, NEG_BIG, F32)
        l_scr[...] = jnp.zeros(l_scr.shape, F32)
        acc_scr[...] = jnp.zeros(acc_scr.shape, F32)

        def step(block, masked, offset=offset):
            start = pl.multiple_of(block * span, span)
            k_win = k_ref[pl.ds(start, span), offset:offset + 256]
            v_win = v_ref[pl.ds(start, span), offset:offset + 256]
            for chain in range(4):
                s = lax.dot_general(q_scr[chain], k_win, (((1,), (1,)), ((), ())), preferred_element_type=F32)
                s = s * scale
                if masked:
                    odd = a_odd if chain % 2 == 0 else 1 - a_odd
                    row = lax.broadcasted_iota(jnp.int32, s.shape, 0) + odd * rows
                    col = lax.broadcasted_iota(jnp.int32, s.shape, 1)
                    s = jnp.where(col <= row, s, NEG_BIG)
                m_old = m_scr[chain]
                m_new = jnp.maximum(m_old, jnp.max(s, axis=1, keepdims=True))
                p = jnp.exp2(s - m_new[:, :1])
                alpha = jnp.exp2(m_old - m_new)
                part_sum = p[:, 0:128]
                for t in range(1, span // 128):
                    part_sum = part_sum + p[:, 128 * t:128 * t + 128]
                l_scr[chain] = l_scr[chain] * alpha + part_sum
                m_scr[chain] = m_new
                pv = jnp.dot(p.astype(BF16), v_win, preferred_element_type=F32)
                acc_scr[chain] = acc_scr[chain] * alpha[:, :1] + pv

        def body(block, carry):
            step(block, False)
            return carry

        lax.fori_loop(0, full_blocks, body, 0)
        step(full_blocks, True)
        outs = []
        for chain in range(4):
            total = jnp.sum(l_scr[chain], axis=1, keepdims=True)
            outs.append(acc_scr[chain] / total)
        split = bounds[0][1]
        window_out.append([
            jnp.where(lane < split, outs[part], outs[2 + part]).astype(BF16) for part in range(2)
        ])
        if window == 0:
            for part, o_ref in ((0, oa_ref), (1, ob_ref)):
                o_ref[:, 0:256] = window_out[0][part]
        else:
            for part, o_ref in ((0, oa_ref), (1, ob_ref)):
                second = window_out[1][part]
                middle = o_ref[:, 128:256]
                o_ref[:, 128:256] = jnp.where(lane[:, :128] < 64, middle, second[:, 0:128])
                o_ref[:, 256:384] = second[:, 128:256]


def attention(info, q_own, q_other, keys, values, head_dim):
    rows = q_own.shape[0]
    length, half = keys.shape
    group = 4 * head_dim
    groups = half // group
    q_own_spec = pl.BlockSpec((rows, group), lambda g, i: (0, i[0] * groups + g))
    col_spec = pl.BlockSpec((rows, group), lambda g, i: (0, g))
    kv_spec = pl.BlockSpec((length, group), lambda g, i: (0, g))
    out = jax.ShapeDtypeStruct((rows, half), BF16)
    scale = head_dim ** -0.5 * LOG2E
    return pl.pallas_call(
        functools.partial(attention_kernel, scale),
        grid_spec=pltpu.PrefetchScalarGridSpec(
            num_scalar_prefetch=1,
            grid=(groups,),
            in_specs=[q_own_spec, col_spec, kv_spec, kv_spec],
            out_specs=[col_spec, col_spec],
            scratch_shapes=[
                pltpu.VMEM((4, rows, 256), BF16),
                pltpu.VMEM((4, rows, 128), F32),
                pltpu.VMEM((4, rows, 128), F32),
                pltpu.VMEM((4, rows, 256), F32),
            ],
        ),
        out_shape=[out, out],
        cost_estimate=pl.CostEstimate(
            flops=8 * rows * length * half, bytes_accessed=4 * length * half, transcendentals=2 * rows * length * 16
        ),
        name="attention",
    )(info, q_own, q_other, keys, values)


def norm_into(dst_ref, src_ref, gain_ref):
    rows = src_ref.shape[0]
    gain = gain_ref[...].astype(F32)

    def body(i, carry):
        sl = pl.ds(pl.multiple_of(i * 32, 32), 32)
        wide = src_ref[sl, :].astype(F32)
        inv = lax.rsqrt(jnp.mean(wide * wide, axis=-1, keepdims=True) + 1e-6)
        dst_ref[sl, :] = (wide * inv * gain).astype(BF16)
        return carry

    lax.fori_loop(0, rows // 32, body, 0)


def query_kernel(layer, x_ref, gain_ref, wq_ref, q_ref, normed, ring, sems):
    width = x_ref.shape[1]
    tiles = q_ref.shape[1] // COLS

    def copy(t):
        return pltpu.make_async_copy(
            wq_ref.at[layer, :, pl.ds(pl.multiple_of(t * COLS, COLS), COLS)], ring.at[lax.rem(t, LOOKAHEAD)], sems.at[lax.rem(t, LOOKAHEAD)]
        )

    for t in range(LOOKAHEAD):
        copy(t).start()
    norm_into(normed, x_ref, gain_ref)

    def body(t, carry):
        copy(t).wait()
        out = jnp.dot(normed[...], ring[lax.rem(t, LOOKAHEAD)], preferred_element_type=F32)
        q_ref[:, pl.ds(pl.multiple_of(t * COLS, COLS), COLS)] = out.astype(BF16)

        @pl.when(t + LOOKAHEAD < tiles)
        def _():
            copy(t + LOOKAHEAD).start()

        return carry

    lax.fori_loop(0, tiles, body, 0)


def query_project(x, gain, w_q, layer):
    rows, width = x.shape
    vmem = pl.BlockSpec(memory_space=pltpu.VMEM)
    return pl.pallas_call(
        functools.partial(query_kernel, layer),
        in_specs=[vmem, vmem, pl.BlockSpec(memory_space=pl.ANY)],
        out_specs=vmem,
        out_shape=jax.ShapeDtypeStruct((rows, w_q.shape[2]), BF16),
        scratch_shapes=[
            pltpu.VMEM((rows, width), BF16),
            pltpu.VMEM((LOOKAHEAD, width, COLS), BF16),
            pltpu.SemaphoreType.DMA((LOOKAHEAD,)),
        ],
        cost_estimate=pl.CostEstimate(flops=2 * rows * width * width, bytes_accessed=2 * width * width, transcendentals=0),
        name="query_project",
    )(x, gain, w_q)


def layer_kernel(
    layer, has_next, core_ref, oa_ref, ob_ref, cur_ref, g_mlp_ref, g_next_ref, wo_ref, wg_ref, wu_ref, wd_ref, wq_ref,
    *refs,
):
    if has_next:
        out_ref, q_ref, mixed, normed, inner, ring, ring_down, sems = refs
    else:
        out_ref, mixed, normed, inner, ring, ring_down, sems = refs
        q_ref = None
    rows, width = cur_ref.shape
    hidden = wg_ref.shape[2]
    n_out = width // COLS
    n_up = hidden // COLS
    n_down = width // DOWN_COLS
    first_up = n_out
    first_down = n_out + 2 * n_up
    first_q = first_down + n_down
    total = first_q + (n_out if has_next else 0)

    def cols(i, size):
        return pl.ds(pl.multiple_of(i * size, size), size)

    def start(t):
        slot = lax.rem(t, LOOKAHEAD)

        def to_ring(src):
            pltpu.make_async_copy(src, ring.at[slot], sems.at[slot]).start()

        @pl.when(t < first_up)
        def _():
            to_ring(wo_ref.at[layer, :, cols(t, COLS)])

        u = t - first_up
        is_up = (t >= first_up) & (t < first_down)

        @pl.when(is_up & (lax.rem(u, 2) == 0))
        def _():
            to_ring(wg_ref.at[layer, :, cols(u // 2, COLS)])

        @pl.when(is_up & (lax.rem(u, 2) == 1))
        def _():
            to_ring(wu_ref.at[layer, :, cols(u // 2, COLS)])

        @pl.when((t >= first_down) & (t < first_q))
        def _():
            pltpu.make_async_copy(
                wd_ref.at[layer, :, cols(t - first_down, DOWN_COLS)], ring_down.at[slot], sems.at[slot]
            ).start()

        if has_next:
            @pl.when((t >= first_q) & (t < total))
            def _():
                to_ring(wq_ref.at[layer + 1, :, cols(t - first_q, COLS)])

    def take(t):
        slot = lax.rem(t, LOOKAHEAD)
        pltpu.make_async_copy(wo_ref.at[layer, :, pl.ds(0, COLS)], ring.at[slot], sems.at[slot]).wait()
        return slot

    for t in range(LOOKAHEAD):
        start(jnp.int32(t))
    core = core_ref[0]
    half = oa_ref.shape[1]
    mixed[:, cols(core, half)] = oa_ref[...]
    mixed[:, cols(1 - core, half)] = ob_ref[...]

    def out_body(t, carry):
        slot = take(t)
        attn = jnp.dot(mixed[...], ring[slot], preferred_element_type=F32).astype(BF16)
        out_ref[:, cols(t, COLS)] = (cur_ref[:, cols(t, COLS)].astype(F32) + attn.astype(F32)).astype(BF16)
        start(t + LOOKAHEAD)
        return carry

    lax.fori_loop(0, n_out, out_body, 0)
    norm_into(normed, out_ref, g_mlp_ref)

    def up_body(j, carry):
        t = first_up + 2 * j
        slot = take(t)
        gate = jnp.dot(normed[...], ring[slot], preferred_element_type=F32).astype(BF16)
        inner[:, cols(j, COLS)] = gate
        start(t + LOOKAHEAD)
        slot = take(t + 1)
        up = jnp.dot(normed[...], ring[slot], preferred_element_type=F32).astype(BF16)
        g = inner[:, cols(j, COLS)].astype(F32)
        inner[:, cols(j, COLS)] = (jax.nn.silu(g) * up.astype(F32)).astype(BF16)
        start(t + 1 + LOOKAHEAD)
        return carry

    lax.fori_loop(0, n_up, up_body, 0)

    def down_body(j, carry):
        t = first_down + j
        slot = lax.rem(t, LOOKAHEAD)
        pltpu.make_async_copy(wd_ref.at[layer, :, pl.ds(0, DOWN_COLS)], ring_down.at[slot], sems.at[slot]).wait()
        down = jnp.dot(inner[...], ring_down[slot], preferred_element_type=F32).astype(BF16)
        sl = cols(j, DOWN_COLS)
        out_ref[:, sl] = (out_ref[:, sl].astype(F32) + down.astype(F32)).astype(BF16)
        start(t + LOOKAHEAD)
        return carry

    lax.fori_loop(0, n_down, down_body, 0)
    if has_next:
        norm_into(normed, out_ref, g_next_ref)

        def q_body(j, carry):
            t = first_q + j
            slot = take(t)
            q_ref[:, cols(j, COLS)] = jnp.dot(normed[...], ring[slot], preferred_element_type=F32).astype(BF16)
            start(t + LOOKAHEAD)
            return carry

        lax.fori_loop(0, n_out, q_body, 0)


def layer_dense(core, o_own, o_other, current, g_mlp, g_next, w_o, w_gate, w_up, w_down, w_q, layer, has_next):
    rows, width = current.shape
    hidden = w_gate.shape[2]
    vmem = pl.BlockSpec(memory_space=pltpu.VMEM)
    hbm = pl.BlockSpec(memory_space=pl.ANY)
    row_out = jax.ShapeDtypeStruct((rows, width), BF16)
    n_outs = 2 if has_next else 1
    macs = rows * width * ((2 if has_next else 1) * width + 3 * hidden)
    return pl.pallas_call(
        functools.partial(layer_kernel, layer, has_next),
        in_specs=[pl.BlockSpec(memory_space=pltpu.SMEM)] + [vmem] * 5 + [hbm] * 5,
        out_specs=[vmem] * n_outs,
        out_shape=[row_out] * n_outs,
        scratch_shapes=[
            pltpu.VMEM((rows, width), BF16),
            pltpu.VMEM((rows, width), BF16),
            pltpu.VMEM((rows, hidden), BF16),
            pltpu.VMEM((LOOKAHEAD, width, COLS), BF16),
            pltpu.VMEM((LOOKAHEAD, hidden, DOWN_COLS), BF16),
            pltpu.SemaphoreType.DMA((LOOKAHEAD,)),
        ],
        compiler_params=pltpu.CompilerParams(vmem_limit_bytes=60 * 1024 * 1024),
        cost_estimate=pl.CostEstimate(flops=2 * macs, bytes_accessed=2 * macs // rows, transcendentals=rows * hidden),
        name="layer_dense",
    )(core, o_own, o_other, current, g_mlp, g_next, w_o, w_gate, w_up, w_down, w_q)


def solution(mesh):
    seq_axes = ('sp', 'cp')
    cp_size = mesh.shape['cp']
    devices = mesh.shape['sp'] * cp_size
    row_spec = P(('dp', 'sp', 'cp'), None)
    pairs = [(i, i ^ 1) for i in range(cp_size)]

    def local(hidden, g_kv, w_k, w_v, g_attn, g_mlp, w_q, w_o, w_gate, w_up, w_down):
        rows, width = hidden.shape
        num_layers, n_heads, head_dim = w_o.shape[0], w_o.shape[1], w_o.shape[2]
        half = w_k.shape[1] // 2
        w_o = w_o.reshape(num_layers, n_heads * head_dim, width)
        index = lax.axis_index('sp') * cp_size + lax.axis_index('cp')
        core_id = lax.rem(index, 2).astype(jnp.int32)
        core = core_id.reshape(1)
        info = jnp.stack([core_id, (index // 2).astype(jnp.int32), core_id])

        normed = rms_norm(hidden, g_kv)
        part = rows // KV_CHUNKS
        gathered = [
            lax.all_gather(normed[c * part:(c + 1) * part], seq_axes, axis=0, tiled=True) for c in range(KV_CHUNKS)
        ]
        query = query_project(hidden, g_attn[0:1], w_q, 0)
        kv = None
        for c in range(KV_CHUNKS):
            kv = kv_project(core, gathered[c], w_k, w_v, c, devices, kv)
        keys, values = (a.reshape(devices * rows, half) for a in kv)

        def swap(full_or_half):
            return lax.ppermute(full_or_half, 'cp', pairs)

        current = hidden
        for layer in range(num_layers):
            q_send = lax.dynamic_slice_in_dim(query, (1 - core_id) * half, half, axis=1)
            q_other = swap(q_send)
            o_own, o_send = attention(info, query, q_other, keys, values, head_dim)
            o_other = swap(o_send)
            has_next = layer + 1 < num_layers
            nxt = layer + 1 if has_next else layer
            outs = layer_dense(
                core, o_own, o_other, current, g_mlp[layer:layer + 1], g_attn[nxt:nxt + 1],
                w_o, w_gate, w_up, w_down, w_q, layer, has_next,
            )
            current = outs[0]
            if has_next:
                query = outs[1]
        return current

    return jax.shard_map(local, mesh=mesh, in_specs=(row_spec,) + (P(),) * 10, out_specs=row_spec, check_vma=False)
```

```python
import functools

import jax
import jax.numpy as jnp
from jax import lax
from jax.experimental import pallas as pl
from jax.experimental.pallas import tpu as pltpu
from jax.sharding import PartitionSpec as P

F32 = jnp.float32
BF16 = jnp.bfloat16
MESH = pl.DeviceIdType.MESH
NEG_BIG = -1e30
LOOKAHEAD = 4
WIDE = 768
COLS = 512
DOWN_COLS = 256
LOG2E = 1.4426950408889634
VMEM_LIMIT = 60 * 1024 * 1024


def cols(i, size):
    return pl.ds(pl.multiple_of(i * size, size), size)


def my_index(cp_size):
    return lax.axis_index('sp') * cp_size + lax.axis_index('cp')


def device(i, cp_size):
    return {'sp': i // cp_size, 'cp': lax.rem(i, cp_size)}


def barrier_signal(n, cp_size):
    me = my_index(cp_size)
    barrier = pltpu.get_barrier_semaphore()

    def body(k, carry):
        peer = lax.rem(me + k, n)
        pl.semaphore_signal(barrier, inc=1, device_id=device(peer, cp_size), device_id_type=MESH)
        return carry

    lax.fori_loop(1, n, body, 0)


def barrier_wait(n):
    pl.semaphore_wait(pltpu.get_barrier_semaphore(), n - 1)


def remote(src, dst, send_sem, recv_sem, peer, cp_size):
    return pltpu.make_async_remote_copy(
        src_ref=src, dst_ref=dst, send_sem=send_sem, recv_sem=recv_sem, device_id=device(peer, cp_size), device_id_type=MESH
    )


def send_block(src_of, dst_of, send_sem, recv_sem, local_sem, peer, me, cp_size):
    @pl.when(peer != me)
    def _():
        remote(src_of(peer), dst_of(me), send_sem.at[peer], recv_sem.at[me], peer, cp_size).start()

    @pl.when(peer == me)
    def _():
        pltpu.make_async_copy(src_of(me), dst_of(me), local_sem).start()


def finish_blocks(src_of, dst_of, send_sem, recv_sem, local_sem, me, n, cp_size):
    pltpu.make_async_copy(src_of(me), dst_of(me), local_sem).wait()

    def body(k, carry):
        peer = lax.rem(me + k, n)
        remote(src_of(peer), dst_of(peer), send_sem.at[peer], recv_sem.at[peer], peer, cp_size).wait_send()
        remote(src_of(peer), dst_of(peer), send_sem.at[peer], recv_sem.at[peer], peer, cp_size).wait_recv()
        return carry

    lax.fori_loop(1, n, body, 0)


def norm_into(dst_ref, src_ref, gain_ref):
    rows = src_ref.shape[0]
    gain = gain_ref[...].astype(F32)

    def body(i, carry):
        sl = pl.ds(pl.multiple_of(i * 32, 32), 32)
        wide = src_ref[sl, :].astype(F32)
        inv = lax.rsqrt(jnp.mean(wide * wide, axis=-1, keepdims=True) + 1e-6)
        dst_ref[sl, :] = (wide * inv * gain).astype(BF16)
        return carry

    lax.fori_loop(0, rows // 32, body, 0)


def transposed_tile(normed, weight, buf_of, first):
    out = jnp.dot(normed, weight, preferred_element_type=F32).astype(BF16).T
    size = out.shape[0] // 4
    for j in range(4):
        buf_of(first + j)[...] = out[j * size:(j + 1) * size]


def first_kernel(
    n, cp_size, x_ref, g_kv_ref, g_q_ref, wk_ref, wv_ref, wq_ref, kv_ref, q_ref,
    normed, normed_q, ring, buf, sems, send_sem, recv_sem, local_sem,
):
    me = my_index(cp_size)
    barrier_signal(n, cp_size)
    per = x_ref.shape[1] // WIDE

    def tile_of(t):
        return lax.rem(t + me // cp_size + 1, per)

    def start(t):
        slot = lax.rem(t, LOOKAHEAD)
        for i, w_ref in enumerate((wk_ref, wv_ref)):
            @pl.when(t // per == i)
            def _(w_ref=w_ref):
                pltpu.make_async_copy(w_ref.at[:, cols(tile_of(t), WIDE)], ring.at[slot], sems.at[slot]).start()

        @pl.when(t // per == 2)
        def _():
            pltpu.make_async_copy(wq_ref.at[0, :, cols(tile_of(t), WIDE)], ring.at[slot], sems.at[slot]).start()

    def dst_of(tensor):
        def of(i):
            return q_ref.at[i] if tensor == 2 else kv_ref.at[tensor, i]

        return of

    def send(tensor, t):
        for j in range(4):
            send_block(
                lambda i: buf.at[tensor, i], dst_of(tensor), send_sem.at[tensor], recv_sem.at[tensor],
                local_sem.at[tensor], 4 * tile_of(t) + j, me, cp_size,
            )

    for t in range(LOOKAHEAD):
        start(jnp.int32(t))
    norm_into(normed, x_ref, g_kv_ref)
    norm_into(normed_q, x_ref, g_q_ref)
    barrier_wait(n)
    for tensor in range(3):
        source = normed_q if tensor == 2 else normed

        def body(i, carry, tensor=tensor, source=source):
            t = tensor * per + i
            slot = lax.rem(t, LOOKAHEAD)
            pltpu.make_async_copy(wk_ref.at[:, pl.ds(0, WIDE)], ring.at[slot], sems.at[slot]).wait()
            transposed_tile(source[...], ring[slot], lambda g: buf.at[tensor, g], 4 * tile_of(t))

            @pl.when(i > 0)
            def _():
                send(tensor, t - 1)

            start(t + LOOKAHEAD)
            return carry

        lax.fori_loop(0, per, body, 0)
        if tensor > 0:
            send(tensor - 1, jnp.int32(tensor * per - 1))
    send(2, jnp.int32(3 * per - 1))
    for tensor in range(3):
        finish_blocks(
            lambda i, tensor=tensor: buf.at[tensor, i], dst_of(tensor), send_sem.at[tensor], recv_sem.at[tensor],
            local_sem.at[tensor], me, n, cp_size,
        )


def first_project(n, cp_size, x, g_kv, g_q, w_k, w_v, w_q):
    rows, width = x.shape
    part = width // n
    vmem = pl.BlockSpec(memory_space=pltpu.VMEM)
    hbm = pl.BlockSpec(memory_space=pl.ANY)
    return pl.pallas_call(
        functools.partial(first_kernel, n, cp_size),
        in_specs=[vmem] * 3 + [hbm] * 3,
        out_specs=[hbm] * 2,
        out_shape=[jax.ShapeDtypeStruct((2, n, part, rows), BF16), jax.ShapeDtypeStruct((n, part, rows), BF16)],
        scratch_shapes=[
            pltpu.VMEM((rows, width), BF16),
            pltpu.VMEM((rows, width), BF16),
            pltpu.VMEM((LOOKAHEAD, width, WIDE), BF16),
            pltpu.VMEM((3, n, part, rows), BF16),
            pltpu.SemaphoreType.DMA((LOOKAHEAD,)),
            pltpu.SemaphoreType.DMA((3, n)),
            pltpu.SemaphoreType.DMA((3, n)),
            pltpu.SemaphoreType.DMA((3,)),
        ],
        compiler_params=pltpu.CompilerParams(collective_id=0, has_side_effects=True, vmem_limit_bytes=VMEM_LIMIT),
        cost_estimate=pl.CostEstimate(flops=6 * rows * width * width, bytes_accessed=6 * width * width, transcendentals=0),
        name="first_project",
    )(x, g_kv, g_q, w_k, w_v, w_q)


def attention_kernel(
    n, cp_size, head_dim, q_ref, kv_ref, o_ref, k_nat, m_scr, l_scr, acc_scr, buf, send_sem, recv_sem, local_sem
):
    me = my_index(cp_size)
    barrier_signal(n, cp_size)
    rows = q_ref.shape[2]
    heads = q_ref.shape[1] // head_dim
    span = 2 * rows
    scale = head_dim ** -0.5 * LOG2E

    def flip(u, carry):
        for h in range(heads):
            block = kv_ref[0, u, h * head_dim:(h + 1) * head_dim, :]
            k_nat[h, cols(u, rows), :] = block.T
        return carry

    lax.fori_loop(0, n, flip, 0)
    barrier_wait(n)

    def src_of(i):
        return buf.at[i]

    def dst_of(i):
        return o_ref.at[i]

    def step(t, pair, masked):
        for h in range(heads):
            hs = slice(h * head_dim, (h + 1) * head_dim)
            q_t = q_ref[t, hs, :]
            s = jnp.dot(k_nat[h, cols(pair, span), :], q_t, preferred_element_type=F32) * scale
            if masked:
                key = lax.broadcasted_iota(jnp.int32, s.shape, 0) + pair * span
                query = lax.broadcasted_iota(jnp.int32, s.shape, 1) + t * rows
                s = jnp.where(key <= query, s, NEG_BIG)
            m_old = m_scr[h]
            m_new = jnp.maximum(m_old, jnp.max(s, axis=0, keepdims=True))
            p = jnp.exp2(s - m_new[0:1])
            alpha = jnp.exp2(m_old - m_new)
            m_scr[h] = m_new
            l_scr[h] = l_scr[h] * alpha + jnp.sum(p.reshape(span // 8, 8, rows), axis=0)
            p = p.astype(BF16)
            pv = jnp.dot(kv_ref[1, 2 * pair, hs, :], p[:rows], preferred_element_type=F32)
            pv = pv + jnp.dot(kv_ref[1, 2 * pair + 1, hs, :], p[rows:], preferred_element_type=F32)
            acc_scr[h] = acc_scr[h] * alpha[0:1] + pv

    def block(k, carry):
        t = lax.rem(me + 1 + k, n)
        m_scr[...] = jnp.full(m_scr.shape, NEG_BIG, F32)
        l_scr[...] = jnp.zeros(l_scr.shape, F32)
        acc_scr[...] = jnp.zeros(acc_scr.shape, F32)

        def body(pair, carry):
            step(t, pair, False)
            return carry

        lax.fori_loop(0, t // 2, body, 0)

        @pl.when(k > 0)
        def _():
            send_block(src_of, dst_of, send_sem, recv_sem, local_sem, lax.rem(me + k, n), me, cp_size)

        step(t, t // 2, True)
        for h in range(heads):
            total = jnp.sum(l_scr[h], axis=0, keepdims=True)
            buf[t, h * head_dim:(h + 1) * head_dim, :] = (acc_scr[h] / total).astype(BF16)
        return carry

    lax.fori_loop(0, n, block, 0)
    send_block(src_of, dst_of, send_sem, recv_sem, local_sem, me, me, cp_size)
    finish_blocks(src_of, dst_of, send_sem, recv_sem, local_sem, me, n, cp_size)


def attention(n, cp_size, head_dim, q, kv, collective_id):
    part, rows = q.shape[1], q.shape[2]
    heads = part // head_dim
    vmem = pl.BlockSpec(memory_space=pltpu.VMEM)
    return pl.pallas_call(
        functools.partial(attention_kernel, n, cp_size, head_dim),
        in_specs=[vmem, vmem],
        out_specs=pl.BlockSpec(memory_space=pl.ANY),
        out_shape=jax.ShapeDtypeStruct(q.shape, BF16),
        scratch_shapes=[
            pltpu.VMEM((heads, n * rows, head_dim), BF16),
            pltpu.VMEM((heads, 8, rows), F32),
            pltpu.VMEM((heads, 8, rows), F32),
            pltpu.VMEM((heads, head_dim, rows), F32),
            pltpu.VMEM(q.shape, BF16),
            pltpu.SemaphoreType.DMA((n,)),
            pltpu.SemaphoreType.DMA((n,)),
            pltpu.SemaphoreType.DMA,
        ],
        compiler_params=pltpu.CompilerParams(
            collective_id=collective_id, has_side_effects=True, vmem_limit_bytes=VMEM_LIMIT
        ),
        cost_estimate=pl.CostEstimate(
            flops=2 * n * n * rows * rows * part, bytes_accessed=8 * n * part * rows, transcendentals=n * n * rows * rows
        ),
        name="attention",
    )(q, kv)


def layer_kernel(
    n, cp_size, layer, has_next, ot_ref, cur_ref, g_mlp_ref, g_next_ref, wo_ref, wg_ref, wu_ref, wd_ref, wq_ref, *refs
):
    if has_next:
        out_ref, q_ref, mixed, inner, ring, ring_down, sems, buf, send_sem, recv_sem, local_sem = refs
    else:
        out_ref, mixed, inner, ring, ring_down, sems = refs
    normed = mixed
    rows, width = cur_ref.shape
    hidden = wg_ref.shape[2]
    per = width // WIDE
    n_up = hidden // COLS
    n_down = width // DOWN_COLS
    first_up = per
    first_down = per + 2 * n_up
    first_q = first_down + n_down
    total = first_q + (per if has_next else 0)
    if has_next:
        me = my_index(cp_size)
        barrier_signal(n, cp_size)

    def tile_of(i):
        return lax.rem(i + me // cp_size + 1, per)

    def start(t):
        slot = lax.rem(t, LOOKAHEAD)
        narrow = ring.at[slot, :, pl.ds(0, COLS)]

        @pl.when(t < first_up)
        def _():
            pltpu.make_async_copy(wo_ref.at[layer, :, cols(t, WIDE)], ring.at[slot], sems.at[slot]).start()

        u = t - first_up
        is_up = (t >= first_up) & (t < first_down)

        @pl.when(is_up & (lax.rem(u, 2) == 0))
        def _():
            pltpu.make_async_copy(wg_ref.at[layer, :, cols(u // 2, COLS)], narrow, sems.at[slot]).start()

        @pl.when(is_up & (lax.rem(u, 2) == 1))
        def _():
            pltpu.make_async_copy(wu_ref.at[layer, :, cols(u // 2, COLS)], narrow, sems.at[slot]).start()

        @pl.when((t >= first_down) & (t < first_q))
        def _():
            pltpu.make_async_copy(
                wd_ref.at[layer, :, cols(t - first_down, DOWN_COLS)], ring_down.at[slot], sems.at[slot]
            ).start()

        if has_next:
            @pl.when((t >= first_q) & (t < total))
            def _():
                pltpu.make_async_copy(
                    wq_ref.at[layer + 1, :, cols(tile_of(t - first_q), WIDE)], ring.at[slot], sems.at[slot]
                ).start()

    def take_wide(t):
        slot = lax.rem(t, LOOKAHEAD)
        pltpu.make_async_copy(wo_ref.at[layer, :, pl.ds(0, WIDE)], ring.at[slot], sems.at[slot]).wait()
        return ring[slot]

    def take(t):
        slot = lax.rem(t, LOOKAHEAD)
        narrow = ring.at[slot, :, pl.ds(0, COLS)]
        pltpu.make_async_copy(wg_ref.at[layer, :, pl.ds(0, COLS)], narrow, sems.at[slot]).wait()
        return narrow[...]

    for t in range(LOOKAHEAD):
        start(jnp.int32(t))

    def flip(i, carry):
        mixed[:, cols(i, 256)] = ot_ref[cols(i, 256), :].T
        return carry

    lax.fori_loop(0, width // 256, flip, 0)

    def out_body(t, carry):
        attn = jnp.dot(mixed[...], take_wide(t), preferred_element_type=F32).astype(BF16)
        out_ref[:, cols(t, WIDE)] = (cur_ref[:, cols(t, WIDE)].astype(F32) + attn.astype(F32)).astype(BF16)
        start(t + LOOKAHEAD)
        return carry

    lax.fori_loop(0, per, out_body, 0)
    norm_into(normed, out_ref, g_mlp_ref)

    def up_body(j, carry):
        t = first_up + 2 * j
        inner[:, cols(j, COLS)] = jnp.dot(normed[...], take(t), preferred_element_type=F32).astype(BF16)
        start(t + LOOKAHEAD)
        up = jnp.dot(normed[...], take(t + 1), preferred_element_type=F32).astype(BF16)
        g = inner[:, cols(j, COLS)].astype(F32)
        inner[:, cols(j, COLS)] = (jax.nn.silu(g) * up.astype(F32)).astype(BF16)
        start(t + 1 + LOOKAHEAD)
        return carry

    lax.fori_loop(0, n_up, up_body, 0)

    def down_body(j, carry):
        t = first_down + j
        slot = lax.rem(t, LOOKAHEAD)
        pltpu.make_async_copy(wd_ref.at[layer, :, pl.ds(0, DOWN_COLS)], ring_down.at[slot], sems.at[slot]).wait()
        down = jnp.dot(inner[...], ring_down[slot], preferred_element_type=F32).astype(BF16)
        sl = cols(j, DOWN_COLS)
        out_ref[:, sl] = (out_ref[:, sl].astype(F32) + down.astype(F32)).astype(BF16)
        start(t + LOOKAHEAD)
        return carry

    lax.fori_loop(0, n_down, down_body, 0)
    if has_next:
        norm_into(normed, out_ref, g_next_ref)
        barrier_wait(n)

        def src_of(i):
            return buf.at[i]

        def dst_of(i):
            return q_ref.at[i]

        def send(i):
            for j in range(4):
                send_block(src_of, dst_of, send_sem, recv_sem, local_sem, 4 * tile_of(i) + j, me, cp_size)

        def q_body(i, carry):
            transposed_tile(normed[...], take_wide(first_q + i), src_of, 4 * tile_of(i))

            @pl.when(i > 0)
            def _():
                send(i - 1)

            return carry

        lax.fori_loop(0, per, q_body, 0)
        send(jnp.int32(per - 1))
        finish_blocks(src_of, dst_of, send_sem, recv_sem, local_sem, me, n, cp_size)


def layer_dense(n, cp_size, o_t, current, g_mlp, g_next, w_o, w_gate, w_up, w_down, w_q, layer, has_next, collective_id):
    rows, width = current.shape
    hidden = w_gate.shape[2]
    part = width // n
    vmem = pl.BlockSpec(memory_space=pltpu.VMEM)
    hbm = pl.BlockSpec(memory_space=pl.ANY)
    out_shape = [jax.ShapeDtypeStruct((rows, width), BF16)]
    out_specs = [vmem]
    scratch = [
        pltpu.VMEM((rows, width), BF16),
        pltpu.VMEM((rows, hidden), BF16),
        pltpu.VMEM((LOOKAHEAD, width, WIDE), BF16),
        pltpu.VMEM((LOOKAHEAD, hidden, DOWN_COLS), BF16),
        pltpu.SemaphoreType.DMA((LOOKAHEAD,)),
    ]
    params = dict(vmem_limit_bytes=VMEM_LIMIT)
    if has_next:
        out_shape.append(jax.ShapeDtypeStruct((n, part, rows), BF16))
        out_specs.append(hbm)
        scratch += [
            pltpu.VMEM((n, part, rows), BF16),
            pltpu.SemaphoreType.DMA((n,)),
            pltpu.SemaphoreType.DMA((n,)),
            pltpu.SemaphoreType.DMA,
        ]
        params.update(collective_id=collective_id, has_side_effects=True)
    macs = rows * width * ((2 if has_next else 1) * width + 3 * hidden)
    return pl.pallas_call(
        functools.partial(layer_kernel, n, cp_size, layer, has_next),
        in_specs=[vmem] * 4 + [hbm] * 5,
        out_specs=out_specs,
        out_shape=out_shape,
        scratch_shapes=scratch,
        compiler_params=pltpu.CompilerParams(**params),
        cost_estimate=pl.CostEstimate(flops=2 * macs, bytes_accessed=2 * macs // rows, transcendentals=rows * hidden),
        name="layer_dense",
    )(o_t, current, g_mlp, g_next, w_o, w_gate, w_up, w_down, w_q)


def solution(mesh):
    cp_size = mesh.shape['cp']
    n = mesh.shape['sp'] * cp_size
    row_spec = P(('dp', 'sp', 'cp'), None)

    def local(hidden, g_kv, w_k, w_v, g_attn, g_mlp, w_q, w_o, w_gate, w_up, w_down):
        rows, width = hidden.shape
        num_layers, n_heads, head_dim = w_o.shape[0], w_o.shape[1], w_o.shape[2]
        w_o = w_o.reshape(num_layers, n_heads * head_dim, width)
        kv, query = first_project(n, cp_size, hidden, g_kv.reshape(1, width), g_attn[0:1], w_k, w_v, w_q)
        current = hidden
        for layer in range(num_layers):
            o_t = attention(n, cp_size, head_dim, query, kv, 2 * layer + 1).reshape(width, rows)
            has_next = layer + 1 < num_layers
            nxt = layer + 1 if has_next else layer
            outs = layer_dense(
                n, cp_size, o_t, current, g_mlp[layer:layer + 1], g_attn[nxt:nxt + 1],
                w_o, w_gate, w_up, w_down, w_q, layer, has_next, 2 * layer + 2,
            )
            current = outs[0]
            if has_next:
                query = outs[1]
        return current

    return jax.shard_map(local, mesh=mesh, in_specs=(row_spec,) + (P(),) * 10, out_specs=row_spec, check_vma=False)
```

```python
import functools

import jax
import jax.numpy as jnp
from jax import lax
from jax.experimental import pallas as pl
from jax.experimental.pallas import tpu as pltpu
from jax.sharding import PartitionSpec as P

F32 = jnp.float32
BF16 = jnp.bfloat16
MESH = pl.DeviceIdType.MESH
NEG_BIG = -1e30
LOOKAHEAD = 4
WIDE = 768
COLS = 512
DOWN_COLS = 256
LOG2E = 1.4426950408889634
VMEM_LIMIT = 60 * 1024 * 1024


def cols(i, size):
    return pl.ds(pl.multiple_of(i * size, size), size)


def my_index(cp_size):
    return lax.axis_index('sp') * cp_size + lax.axis_index('cp')


def device(i, cp_size):
    return {'sp': i // cp_size, 'cp': lax.rem(i, cp_size)}


def barrier_signal(n, cp_size):
    me = my_index(cp_size)
    barrier = pltpu.get_barrier_semaphore()

    def body(k, carry):
        peer = lax.rem(me + k, n)
        pl.semaphore_signal(barrier, inc=1, device_id=device(peer, cp_size), device_id_type=MESH)
        return carry

    lax.fori_loop(1, n, body, 0)


def barrier_wait(n):
    pl.semaphore_wait(pltpu.get_barrier_semaphore(), n - 1)


def remote(src, dst, send_sem, recv_sem, peer, cp_size):
    return pltpu.make_async_remote_copy(
        src_ref=src, dst_ref=dst, send_sem=send_sem, recv_sem=recv_sem, device_id=device(peer, cp_size), device_id_type=MESH
    )


def send_block(src_of, dst_of, send_sem, recv_sem, local_sem, peer, me, cp_size):
    @pl.when(peer != me)
    def _():
        remote(src_of(peer), dst_of(me), send_sem.at[peer], recv_sem.at[me], peer, cp_size).start()

    @pl.when(peer == me)
    def _():
        pltpu.make_async_copy(src_of(me), dst_of(me), local_sem).start()


def finish_blocks(src_of, dst_of, send_sem, recv_sem, local_sem, me, n, cp_size):
    pltpu.make_async_copy(src_of(me), dst_of(me), local_sem).wait()

    def body(k, carry):
        peer = lax.rem(me + k, n)
        remote(src_of(peer), dst_of(peer), send_sem.at[peer], recv_sem.at[peer], peer, cp_size).wait_send()
        remote(src_of(peer), dst_of(peer), send_sem.at[peer], recv_sem.at[peer], peer, cp_size).wait_recv()
        return carry

    lax.fori_loop(1, n, body, 0)


def norm_into(dst_ref, src_ref, gain_ref):
    rows = src_ref.shape[0]
    gain = gain_ref[...].astype(F32)

    def body(i, carry):
        sl = pl.ds(pl.multiple_of(i * 32, 32), 32)
        wide = src_ref[sl, :].astype(F32)
        inv = lax.rsqrt(jnp.mean(wide * wide, axis=-1, keepdims=True) + 1e-6)
        dst_ref[sl, :] = (wide * inv * gain).astype(BF16)
        return carry

    lax.fori_loop(0, rows // 32, body, 0)


def transposed_tile(normed, weight, buf_of, first):
    out = jnp.dot(normed, weight, preferred_element_type=F32).astype(BF16).T
    size = out.shape[0] // 4
    for j in range(4):
        buf_of(first + j)[...] = out[j * size:(j + 1) * size]


def first_kernel(
    n, cp_size, x_ref, g_kv_ref, g_q_ref, wk_ref, wv_ref, wq_ref, kv_ref, q_ref,
    normed, normed_q, ring, buf, sems, send_sem, recv_sem, local_sem,
):
    me = my_index(cp_size)
    barrier_signal(n, cp_size)
    per = x_ref.shape[1] // WIDE

    def tile_of(t):
        return lax.rem(t + me // cp_size + 1, per)

    def start(t):
        slot = lax.rem(t, LOOKAHEAD)
        for i, w_ref in enumerate((wk_ref, wv_ref)):
            @pl.when(t // per == i)
            def _(w_ref=w_ref):
                pltpu.make_async_copy(w_ref.at[:, cols(tile_of(t), WIDE)], ring.at[slot], sems.at[slot]).start()

        @pl.when(t // per == 2)
        def _():
            pltpu.make_async_copy(wq_ref.at[0, :, cols(tile_of(t), WIDE)], ring.at[slot], sems.at[slot]).start()

    def dst_of(tensor):
        def of(i):
            return q_ref.at[i] if tensor == 2 else kv_ref.at[tensor, i]

        return of

    def send(tensor, t):
        for j in range(4):
            send_block(
                lambda i: buf.at[tensor, i], dst_of(tensor), send_sem.at[tensor], recv_sem.at[tensor],
                local_sem.at[tensor], 4 * tile_of(t) + j, me, cp_size,
            )

    for t in range(LOOKAHEAD):
        start(jnp.int32(t))
    norm_into(normed, x_ref, g_kv_ref)
    norm_into(normed_q, x_ref, g_q_ref)
    barrier_wait(n)
    for tensor in range(3):
        source = normed_q if tensor == 2 else normed

        def body(i, carry, tensor=tensor, source=source):
            t = tensor * per + i
            slot = lax.rem(t, LOOKAHEAD)
            pltpu.make_async_copy(wk_ref.at[:, pl.ds(0, WIDE)], ring.at[slot], sems.at[slot]).wait()
            transposed_tile(source[...], ring[slot], lambda g: buf.at[tensor, g], 4 * tile_of(t))

            @pl.when(i > 0)
            def _():
                send(tensor, t - 1)

            start(t + LOOKAHEAD)
            return carry

        lax.fori_loop(0, per, body, 0)
        if tensor > 0:
            send(tensor - 1, jnp.int32(tensor * per - 1))
    send(2, jnp.int32(3 * per - 1))
    for tensor in range(3):
        finish_blocks(
            lambda i, tensor=tensor: buf.at[tensor, i], dst_of(tensor), send_sem.at[tensor], recv_sem.at[tensor],
            local_sem.at[tensor], me, n, cp_size,
        )


def first_project(n, cp_size, x, g_kv, g_q, w_k, w_v, w_q):
    rows, width = x.shape
    part = width // n
    vmem = pl.BlockSpec(memory_space=pltpu.VMEM)
    hbm = pl.BlockSpec(memory_space=pl.ANY)
    return pl.pallas_call(
        functools.partial(first_kernel, n, cp_size),
        in_specs=[vmem] * 3 + [hbm] * 3,
        out_specs=[hbm] * 2,
        out_shape=[jax.ShapeDtypeStruct((2, n, part, rows), BF16), jax.ShapeDtypeStruct((n, part, rows), BF16)],
        scratch_shapes=[
            pltpu.VMEM((rows, width), BF16),
            pltpu.VMEM((rows, width), BF16),
            pltpu.VMEM((LOOKAHEAD, width, WIDE), BF16),
            pltpu.VMEM((3, n, part, rows), BF16),
            pltpu.SemaphoreType.DMA((LOOKAHEAD,)),
            pltpu.SemaphoreType.DMA((3, n)),
            pltpu.SemaphoreType.DMA((3, n)),
            pltpu.SemaphoreType.DMA((3,)),
        ],
        compiler_params=pltpu.CompilerParams(collective_id=0, has_side_effects=True, vmem_limit_bytes=VMEM_LIMIT),
        cost_estimate=pl.CostEstimate(flops=6 * rows * width * width, bytes_accessed=6 * width * width, transcendentals=0),
        name="first_project",
    )(x, g_kv, g_q, w_k, w_v, w_q)


def attention_kernel(
    n, cp_size, head_dim, q_ref, kv_ref, o_ref, k_nat, v_all, s_scr, top_scr, max_scr, sum_scr, acc_scr, buf,
    send_sem, recv_sem, local_sem,
):
    me = my_index(cp_size)
    barrier_signal(n, cp_size)
    rows = q_ref.shape[2]
    heads = q_ref.shape[1] // head_dim
    span = 2 * rows
    scale = head_dim ** -0.5 * LOG2E

    def flip(u, carry):
        for h in range(heads):
            hs = slice(h * head_dim, (h + 1) * head_dim)
            k_nat[h, cols(u, rows), :] = kv_ref[0, u, hs, :].T
            v_all[h, :, cols(u, rows)] = kv_ref[1, u, hs, :]
        return carry

    lax.fori_loop(0, n, flip, 0)

    def src_of(i):
        return buf.at[i]

    def dst_of(i):
        return o_ref.at[i]

    def block_of(k):
        return lax.rem(me + 1 + k, n)

    def scores(k, pair, masked):
        t = block_of(k)
        slot = lax.rem(k, 2)
        for h in range(heads):
            q_t = q_ref[t, h * head_dim:(h + 1) * head_dim, :]
            s = jnp.dot(k_nat[h, cols(pair, span), :], q_t, preferred_element_type=F32)
            if masked:
                key = lax.broadcasted_iota(jnp.int32, s.shape, 0) + pair * span
                query = lax.broadcasted_iota(jnp.int32, s.shape, 1) + t * rows
                s = jnp.where(key <= query, s, NEG_BIG)
            s_scr[slot, h, cols(pair, span), :] = s
            top = jnp.max(s.reshape(span // 8, 8, rows), axis=0)
            top_scr[slot, h] = jnp.maximum(top_scr[slot, h], top)

    def values(k, pair):
        slot = lax.rem(k, 2)
        for h in range(heads):
            s = s_scr[slot, h, cols(pair, span), :].reshape(span // 8, 8, rows)
            p = jnp.exp2(s * scale - max_scr[h][None])
            sum_scr[h] = sum_scr[h] + jnp.sum(p, axis=0)
            p = p.reshape(span, rows).astype(BF16)
            acc_scr[h] = acc_scr[h] + jnp.dot(v_all[h, :, cols(pair, span)], p, preferred_element_type=F32)

    def loop(lo, hi, fn):
        def body(pair, carry):
            fn(pair)
            return carry

        lax.fori_loop(lo, hi, body, 0)

    def clear_top(k):
        top_scr[lax.rem(k, 2)] = jnp.full(top_scr.shape[1:], NEG_BIG, F32)

    clear_top(jnp.int32(0))
    loop(0, block_of(0) // 2, lambda pair: scores(0, pair, False))
    scores(0, block_of(0) // 2, True)
    barrier_wait(n)

    def begin_values(k):
        for h in range(heads):
            top = jnp.max(top_scr[lax.rem(k, 2), h], axis=0, keepdims=True) * scale
            max_scr[h] = jnp.broadcast_to(top, max_scr.shape[1:])
        sum_scr[...] = jnp.zeros(sum_scr.shape, F32)
        acc_scr[...] = jnp.zeros(acc_scr.shape, F32)

    def end_values(k):
        for h in range(heads):
            total = jnp.sum(sum_scr[h], axis=0, keepdims=True)
            buf[block_of(k), h * head_dim:(h + 1) * head_dim, :] = (acc_scr[h] / total).astype(BF16)

    def send(k):
        send_block(src_of, dst_of, send_sem, recv_sem, local_sem, block_of(k), me, cp_size)

    def block(k, carry):
        last = block_of(k) // 2
        last_next = block_of(k + 1) // 2
        begin_values(k)
        clear_top(k + 1)
        both = jnp.minimum(last, last_next)

        def fused(pair):
            scores(k + 1, pair, False)
            values(k, pair)

        loop(0, both, fused)

        @pl.when(k > 0)
        def _():
            send(k - 1)

        loop(both, last, lambda pair: values(k, pair))
        loop(both, last_next, lambda pair: scores(k + 1, pair, False))
        scores(k + 1, last_next, True)
        values(k, last)
        end_values(k)
        return carry

    lax.fori_loop(0, n - 1, block, 0)
    begin_values(n - 1)
    send(n - 2)
    loop(0, me // 2 + 1, lambda pair: values(n - 1, pair))
    end_values(n - 1)
    send(n - 1)
    finish_blocks(src_of, dst_of, send_sem, recv_sem, local_sem, me, n, cp_size)


def attention(n, cp_size, head_dim, q, kv, collective_id):
    part, rows = q.shape[1], q.shape[2]
    heads = part // head_dim
    vmem = pl.BlockSpec(memory_space=pltpu.VMEM)
    return pl.pallas_call(
        functools.partial(attention_kernel, n, cp_size, head_dim),
        in_specs=[vmem, vmem],
        out_specs=pl.BlockSpec(memory_space=pl.ANY),
        out_shape=jax.ShapeDtypeStruct(q.shape, BF16),
        scratch_shapes=[
            pltpu.VMEM((heads, n * rows, head_dim), BF16),
            pltpu.VMEM((heads, head_dim, n * rows), BF16),
            pltpu.VMEM((2, heads, n * rows, rows), F32),
            pltpu.VMEM((2, heads, 8, rows), F32),
            pltpu.VMEM((heads, 8, rows), F32),
            pltpu.VMEM((heads, 8, rows), F32),
            pltpu.VMEM((heads, head_dim, rows), F32),
            pltpu.VMEM(q.shape, BF16),
            pltpu.SemaphoreType.DMA((n,)),
            pltpu.SemaphoreType.DMA((n,)),
            pltpu.SemaphoreType.DMA,
        ],
        compiler_params=pltpu.CompilerParams(
            collective_id=collective_id, has_side_effects=True, vmem_limit_bytes=VMEM_LIMIT
        ),
        cost_estimate=pl.CostEstimate(
            flops=2 * n * n * rows * rows * part, bytes_accessed=8 * n * part * rows, transcendentals=n * n * rows * rows
        ),
        name="attention",
    )(q, kv)


def layer_kernel(
    n, cp_size, layer, has_next, ot_ref, cur_ref, g_mlp_ref, g_next_ref, wo_ref, wg_ref, wu_ref, wd_ref, wq_ref, *refs
):
    if has_next:
        out_ref, q_ref, mixed, inner, ring, ring_down, sems, buf, send_sem, recv_sem, local_sem = refs
    else:
        out_ref, mixed, inner, ring, ring_down, sems = refs
    normed = mixed
    rows, width = cur_ref.shape
    hidden = wg_ref.shape[2]
    per = width // WIDE
    n_up = hidden // COLS
    n_down = width // DOWN_COLS
    first_up = per
    first_down = per + 2 * n_up
    first_q = first_down + n_down
    total = first_q + (per if has_next else 0)
    if has_next:
        me = my_index(cp_size)
        barrier_signal(n, cp_size)

    def tile_of(i):
        return lax.rem(i + me // cp_size + 1, per)

    def start(t):
        slot = lax.rem(t, LOOKAHEAD)
        narrow = ring.at[slot, :, pl.ds(0, COLS)]

        @pl.when(t < first_up)
        def _():
            pltpu.make_async_copy(wo_ref.at[layer, :, cols(t, WIDE)], ring.at[slot], sems.at[slot]).start()

        u = t - first_up
        is_up = (t >= first_up) & (t < first_down)

        @pl.when(is_up & (lax.rem(u, 2) == 0))
        def _():
            pltpu.make_async_copy(wg_ref.at[layer, :, cols(u // 2, COLS)], narrow, sems.at[slot]).start()

        @pl.when(is_up & (lax.rem(u, 2) == 1))
        def _():
            pltpu.make_async_copy(wu_ref.at[layer, :, cols(u // 2, COLS)], narrow, sems.at[slot]).start()

        @pl.when((t >= first_down) & (t < first_q))
        def _():
            pltpu.make_async_copy(
                wd_ref.at[layer, :, cols(t - first_down, DOWN_COLS)], ring_down.at[slot], sems.at[slot]
            ).start()

        if has_next:
            @pl.when((t >= first_q) & (t < total))
            def _():
                pltpu.make_async_copy(
                    wq_ref.at[layer + 1, :, cols(tile_of(t - first_q), WIDE)], ring.at[slot], sems.at[slot]
                ).start()

    def take_wide(t):
        slot = lax.rem(t, LOOKAHEAD)
        pltpu.make_async_copy(wo_ref.at[layer, :, pl.ds(0, WIDE)], ring.at[slot], sems.at[slot]).wait()
        return ring[slot]

    def take(t):
        slot = lax.rem(t, LOOKAHEAD)
        narrow = ring.at[slot, :, pl.ds(0, COLS)]
        pltpu.make_async_copy(wg_ref.at[layer, :, pl.ds(0, COLS)], narrow, sems.at[slot]).wait()
        return narrow[...]

    for t in range(LOOKAHEAD):
        start(jnp.int32(t))

    def flip(i, carry):
        mixed[:, cols(i, 256)] = ot_ref[cols(i, 256), :].T
        return carry

    lax.fori_loop(0, width // 256, flip, 0)

    def out_body(t, carry):
        attn = jnp.dot(mixed[...], take_wide(t), preferred_element_type=F32).astype(BF16)
        out_ref[:, cols(t, WIDE)] = (cur_ref[:, cols(t, WIDE)].astype(F32) + attn.astype(F32)).astype(BF16)
        start(t + LOOKAHEAD)
        return carry

    lax.fori_loop(0, per, out_body, 0)
    norm_into(normed, out_ref, g_mlp_ref)

    def up_body(j, carry):
        t = first_up + 2 * j
        inner[:, cols(j, COLS)] = jnp.dot(normed[...], take(t), preferred_element_type=F32).astype(BF16)
        start(t + LOOKAHEAD)
        up = jnp.dot(normed[...], take(t + 1), preferred_element_type=F32).astype(BF16)
        g = inner[:, cols(j, COLS)].astype(F32)
        inner[:, cols(j, COLS)] = (jax.nn.silu(g) * up.astype(F32)).astype(BF16)
        start(t + 1 + LOOKAHEAD)
        return carry

    lax.fori_loop(0, n_up, up_body, 0)

    def down_body(j, carry):
        t = first_down + j
        slot = lax.rem(t, LOOKAHEAD)
        pltpu.make_async_copy(wd_ref.at[layer, :, pl.ds(0, DOWN_COLS)], ring_down.at[slot], sems.at[slot]).wait()
        down = jnp.dot(inner[...], ring_down[slot], preferred_element_type=F32).astype(BF16)
        sl = cols(j, DOWN_COLS)
        out_ref[:, sl] = (out_ref[:, sl].astype(F32) + down.astype(F32)).astype(BF16)
        start(t + LOOKAHEAD)
        return carry

    lax.fori_loop(0, n_down, down_body, 0)
    if has_next:
        norm_into(normed, out_ref, g_next_ref)
        barrier_wait(n)

        def src_of(i):
            return buf.at[i]

        def dst_of(i):
            return q_ref.at[i]

        def send(i):
            for j in range(4):
                send_block(src_of, dst_of, send_sem, recv_sem, local_sem, 4 * tile_of(i) + j, me, cp_size)

        def q_body(i, carry):
            transposed_tile(normed[...], take_wide(first_q + i), src_of, 4 * tile_of(i))

            @pl.when(i > 0)
            def _():
                send(i - 1)

            return carry

        lax.fori_loop(0, per, q_body, 0)
        send(jnp.int32(per - 1))
        finish_blocks(src_of, dst_of, send_sem, recv_sem, local_sem, me, n, cp_size)


def layer_dense(n, cp_size, o_t, current, g_mlp, g_next, w_o, w_gate, w_up, w_down, w_q, layer, has_next, collective_id):
    rows, width = current.shape
    hidden = w_gate.shape[2]
    part = width // n
    vmem = pl.BlockSpec(memory_space=pltpu.VMEM)
    hbm = pl.BlockSpec(memory_space=pl.ANY)
    out_shape = [jax.ShapeDtypeStruct((rows, width), BF16)]
    out_specs = [vmem]
    scratch = [
        pltpu.VMEM((rows, width), BF16),
        pltpu.VMEM((rows, hidden), BF16),
        pltpu.VMEM((LOOKAHEAD, width, WIDE), BF16),
        pltpu.VMEM((LOOKAHEAD, hidden, DOWN_COLS), BF16),
        pltpu.SemaphoreType.DMA((LOOKAHEAD,)),
    ]
    params = dict(vmem_limit_bytes=VMEM_LIMIT)
    if has_next:
        out_shape.append(jax.ShapeDtypeStruct((n, part, rows), BF16))
        out_specs.append(hbm)
        scratch += [
            pltpu.VMEM((n, part, rows), BF16),
            pltpu.SemaphoreType.DMA((n,)),
            pltpu.SemaphoreType.DMA((n,)),
            pltpu.SemaphoreType.DMA,
        ]
        params.update(collective_id=collective_id, has_side_effects=True)
    macs = rows * width * ((2 if has_next else 1) * width + 3 * hidden)
    return pl.pallas_call(
        functools.partial(layer_kernel, n, cp_size, layer, has_next),
        in_specs=[vmem] * 4 + [hbm] * 5,
        out_specs=out_specs,
        out_shape=out_shape,
        scratch_shapes=scratch,
        compiler_params=pltpu.CompilerParams(**params),
        cost_estimate=pl.CostEstimate(flops=2 * macs, bytes_accessed=2 * macs // rows, transcendentals=rows * hidden),
        name="layer_dense",
    )(o_t, current, g_mlp, g_next, w_o, w_gate, w_up, w_down, w_q)


def solution(mesh):
    cp_size = mesh.shape['cp']
    n = mesh.shape['sp'] * cp_size
    row_spec = P(('dp', 'sp', 'cp'), None)

    def local(hidden, g_kv, w_k, w_v, g_attn, g_mlp, w_q, w_o, w_gate, w_up, w_down):
        rows, width = hidden.shape
        num_layers, n_heads, head_dim = w_o.shape[0], w_o.shape[1], w_o.shape[2]
        w_o = w_o.reshape(num_layers, n_heads * head_dim, width)
        kv, query = first_project(n, cp_size, hidden, g_kv.reshape(1, width), g_attn[0:1], w_k, w_v, w_q)
        current = hidden
        for layer in range(num_layers):
            o_t = attention(n, cp_size, head_dim, query, kv, 2 * layer + 1).reshape(width, rows)
            has_next = layer + 1 < num_layers
            nxt = layer + 1 if has_next else layer
            outs = layer_dense(
                n, cp_size, o_t, current, g_mlp[layer:layer + 1], g_attn[nxt:nxt + 1],
                w_o, w_gate, w_up, w_down, w_q, layer, has_next, 2 * layer + 2,
            )
            current = outs[0]
            if has_next:
                query = outs[1]
        return current

    return jax.shard_map(local, mesh=mesh, in_specs=(row_spec,) + (P(),) * 10, out_specs=row_spec, check_vma=False)
```

```python
import functools

import jax
import jax.numpy as jnp
from jax import lax
from jax.experimental import pallas as pl
from jax.experimental.pallas import tpu as pltpu
from jax.sharding import PartitionSpec as P

F32 = jnp.float32
BF16 = jnp.bfloat16
MESH = pl.DeviceIdType.MESH
NEG_BIG = -1e30
LOOKAHEAD = 4
WIDE = 768
COLS = 512
DOWN_COLS = 256
LOG2E = 1.4426950408889634
VMEM_LIMIT = 60 * 1024 * 1024


def cols(i, size):
    return pl.ds(pl.multiple_of(i * size, size), size)


def my_index(cp_size):
    return lax.axis_index('sp') * cp_size + lax.axis_index('cp')


def device(i, cp_size):
    return {'sp': i // cp_size, 'cp': lax.rem(i, cp_size)}


def barrier_signal(n, cp_size):
    me = my_index(cp_size)
    barrier = pltpu.get_barrier_semaphore()

    def body(k, carry):
        peer = lax.rem(me + k, n)
        pl.semaphore_signal(barrier, inc=1, device_id=device(peer, cp_size), device_id_type=MESH)
        return carry

    lax.fori_loop(1, n, body, 0)


def barrier_wait(n):
    pl.semaphore_wait(pltpu.get_barrier_semaphore(), n - 1)


def remote(src, dst, send_sem, recv_sem, peer, cp_size):
    return pltpu.make_async_remote_copy(
        src_ref=src, dst_ref=dst, send_sem=send_sem, recv_sem=recv_sem, device_id=device(peer, cp_size), device_id_type=MESH
    )


def send_block(src_of, dst_of, send_sem, recv_sem, local_sem, peer, me, cp_size):
    @pl.when(peer != me)
    def _():
        remote(src_of(peer), dst_of(me), send_sem.at[peer], recv_sem.at[me], peer, cp_size).start()

    @pl.when(peer == me)
    def _():
        pltpu.make_async_copy(src_of(me), dst_of(me), local_sem).start()


def finish_blocks(src_of, dst_of, send_sem, recv_sem, local_sem, me, n, cp_size):
    pltpu.make_async_copy(src_of(me), dst_of(me), local_sem).wait()

    def body(k, carry):
        peer = lax.rem(me + k, n)
        remote(src_of(peer), dst_of(peer), send_sem.at[peer], recv_sem.at[peer], peer, cp_size).wait_send()
        remote(src_of(peer), dst_of(peer), send_sem.at[peer], recv_sem.at[peer], peer, cp_size).wait_recv()
        return carry

    lax.fori_loop(1, n, body, 0)


def norm_into(dst_ref, src_ref, gain):
    rows = src_ref.shape[0]
    gain = gain.astype(F32)

    def body(i, carry):
        sl = pl.ds(pl.multiple_of(i * 32, 32), 32)
        wide = src_ref[sl, :].astype(F32)
        inv = lax.rsqrt(jnp.mean(wide * wide, axis=-1, keepdims=True) + 1e-6)
        dst_ref[sl, :] = (wide * inv * gain).astype(BF16)
        return carry

    lax.fori_loop(0, rows // 32, body, 0)


def transposed_tile(normed, weight, buf_of, first):
    out = jnp.dot(normed, weight, preferred_element_type=F32).astype(BF16).T
    size = out.shape[0] // 4
    for j in range(4):
        buf_of(first + j)[...] = out[j * size:(j + 1) * size]


def first_kernel(
    n, cp_size, x_ref, g_kv_ref, g_q_ref, wk_ref, wv_ref, wq_ref, kv_ref, q_ref,
    normed, normed_q, ring, buf, sems, send_sem, recv_sem, local_sem,
):
    me = my_index(cp_size)
    barrier_signal(n, cp_size)
    per = x_ref.shape[1] // WIDE

    def tile_of(t):
        return lax.rem(t + me // cp_size + 1, per)

    def start(t):
        slot = lax.rem(t, LOOKAHEAD)
        for i, w_ref in enumerate((wk_ref, wv_ref)):
            @pl.when(t // per == i)
            def _(w_ref=w_ref):
                pltpu.make_async_copy(w_ref.at[:, cols(tile_of(t), WIDE)], ring.at[slot], sems.at[slot]).start()

        @pl.when(t // per == 2)
        def _():
            pltpu.make_async_copy(wq_ref.at[0, :, cols(tile_of(t), WIDE)], ring.at[slot], sems.at[slot]).start()

    def dst_of(tensor):
        def of(i):
            return q_ref.at[i] if tensor == 2 else kv_ref.at[tensor, i]

        return of

    def send(tensor, t):
        for j in range(4):
            send_block(
                lambda i: buf.at[tensor, i], dst_of(tensor), send_sem.at[tensor], recv_sem.at[tensor],
                local_sem.at[tensor], 4 * tile_of(t) + lax.rem(me + j, 4), me, cp_size,
            )

    for t in range(LOOKAHEAD):
        start(jnp.int32(t))
    norm_into(normed, x_ref, g_kv_ref[...].reshape(1, x_ref.shape[1]))
    norm_into(normed_q, x_ref, g_q_ref[0:1, :])
    barrier_wait(n)
    for tensor in range(3):
        source = normed_q if tensor == 2 else normed

        def body(i, carry, tensor=tensor, source=source):
            t = tensor * per + i
            slot = lax.rem(t, LOOKAHEAD)
            pltpu.make_async_copy(wk_ref.at[:, pl.ds(0, WIDE)], ring.at[slot], sems.at[slot]).wait()
            transposed_tile(source[...], ring[slot], lambda g: buf.at[tensor, g], 4 * tile_of(t))

            @pl.when(i > 0)
            def _():
                send(tensor, t - 1)

            start(t + LOOKAHEAD)
            return carry

        lax.fori_loop(0, per, body, 0)
        if tensor > 0:
            send(tensor - 1, jnp.int32(tensor * per - 1))
    send(2, jnp.int32(3 * per - 1))
    for tensor in range(3):
        finish_blocks(
            lambda i, tensor=tensor: buf.at[tensor, i], dst_of(tensor), send_sem.at[tensor], recv_sem.at[tensor],
            local_sem.at[tensor], me, n, cp_size,
        )


def first_project(n, cp_size, x, g_kv, g_q, w_k, w_v, w_q):
    rows, width = x.shape
    part = width // n
    vmem = pl.BlockSpec(memory_space=pltpu.VMEM)
    hbm = pl.BlockSpec(memory_space=pl.ANY)
    return pl.pallas_call(
        functools.partial(first_kernel, n, cp_size),
        in_specs=[vmem] * 3 + [hbm] * 3,
        out_specs=[hbm] * 2,
        out_shape=[jax.ShapeDtypeStruct((2, n, part, rows), BF16), jax.ShapeDtypeStruct((n, part, rows), BF16)],
        scratch_shapes=[
            pltpu.VMEM((rows, width), BF16),
            pltpu.VMEM((rows, width), BF16),
            pltpu.VMEM((LOOKAHEAD, width, WIDE), BF16),
            pltpu.VMEM((3, n, part, rows), BF16),
            pltpu.SemaphoreType.DMA((LOOKAHEAD,)),
            pltpu.SemaphoreType.DMA((3, n)),
            pltpu.SemaphoreType.DMA((3, n)),
            pltpu.SemaphoreType.DMA((3,)),
        ],
        compiler_params=pltpu.CompilerParams(collective_id=0, has_side_effects=True, vmem_limit_bytes=VMEM_LIMIT),
        cost_estimate=pl.CostEstimate(flops=6 * rows * width * width, bytes_accessed=6 * width * width, transcendentals=0),
        name="first_project",
    )(x, g_kv, g_q, w_k, w_v, w_q)


def attention_kernel(
    n, cp_size, head_dim, q_ref, kv_ref, o_ref, k_nat, v_all, s_scr, top_scr, max_scr, sum_scr, acc_scr, buf,
    send_sem, recv_sem, local_sem,
):
    me = my_index(cp_size)
    barrier_signal(n, cp_size)
    rows = q_ref.shape[2]
    heads = q_ref.shape[1] // head_dim
    span = 2 * rows
    scale = head_dim ** -0.5 * LOG2E

    def flip(u, carry):
        for h in range(heads):
            hs = slice(h * head_dim, (h + 1) * head_dim)
            k_nat[h, cols(u, rows), :] = kv_ref[0, u, hs, :].T
            v_all[h, :, cols(u, rows)] = kv_ref[1, u, hs, :]
        return carry

    lax.fori_loop(0, n, flip, 0)

    def src_of(i):
        return buf.at[i]

    def dst_of(i):
        return o_ref.at[i]

    side = n // 2
    mine = me // side

    def block_of(k):
        near = k // side
        return ((1 - mine) * (1 - near) + mine * near) * side + lax.rem(me + k + near, side)

    def scores(k, pair, masked):
        t = block_of(k)
        slot = lax.rem(k, 2)
        for h in range(heads):
            q_t = q_ref[t, h * head_dim:(h + 1) * head_dim, :]
            s = jnp.dot(k_nat[h, cols(pair, span), :], q_t, preferred_element_type=F32)
            if masked:
                key = lax.broadcasted_iota(jnp.int32, s.shape, 0) + pair * span
                query = lax.broadcasted_iota(jnp.int32, s.shape, 1) + t * rows
                s = jnp.where(key <= query, s, NEG_BIG)
            s_scr[slot, h, cols(pair, span), :] = s
            top = jnp.max(s.reshape(span // 8, 8, rows), axis=0)
            top_scr[slot, h] = jnp.maximum(top_scr[slot, h], top)

    def values(k, pair):
        slot = lax.rem(k, 2)
        for h in range(heads):
            s = s_scr[slot, h, cols(pair, span), :].reshape(span // 8, 8, rows)
            p = jnp.exp2(s * scale - max_scr[h][None])
            sum_scr[h] = sum_scr[h] + jnp.sum(p, axis=0)
            p = p.reshape(span, rows).astype(BF16)
            acc_scr[h] = acc_scr[h] + jnp.dot(v_all[h, :, cols(pair, span)], p, preferred_element_type=F32)

    def loop(lo, hi, fn):
        def body(pair, carry):
            fn(pair)
            return carry

        lax.fori_loop(lo, hi, body, 0)

    def clear_top(k):
        top_scr[lax.rem(k, 2)] = jnp.full(top_scr.shape[1:], NEG_BIG, F32)

    clear_top(jnp.int32(0))
    loop(0, block_of(0) // 2, lambda pair: scores(0, pair, False))
    scores(0, block_of(0) // 2, True)
    barrier_wait(n)

    def begin_values(k):
        for h in range(heads):
            top = jnp.max(top_scr[lax.rem(k, 2), h], axis=0, keepdims=True) * scale
            max_scr[h] = jnp.broadcast_to(top, max_scr.shape[1:])
        sum_scr[...] = jnp.zeros(sum_scr.shape, F32)
        acc_scr[...] = jnp.zeros(acc_scr.shape, F32)

    def end_values(k):
        for h in range(heads):
            total = jnp.sum(sum_scr[h], axis=0, keepdims=True)
            buf[block_of(k), h * head_dim:(h + 1) * head_dim, :] = (acc_scr[h] / total).astype(BF16)

    def send(k):
        send_block(src_of, dst_of, send_sem, recv_sem, local_sem, block_of(k), me, cp_size)

    def block(k, carry):
        last = block_of(k) // 2
        last_next = block_of(k + 1) // 2
        begin_values(k)
        clear_top(k + 1)
        both = jnp.minimum(last, last_next)

        def fused(pair):
            scores(k + 1, pair, False)
            values(k, pair)

        loop(0, both, fused)

        @pl.when(k > 0)
        def _():
            send(k - 1)

        loop(both, last, lambda pair: values(k, pair))
        loop(both, last_next, lambda pair: scores(k + 1, pair, False))
        scores(k + 1, last_next, True)
        values(k, last)
        end_values(k)
        return carry

    lax.fori_loop(0, n - 1, block, 0)
    begin_values(n - 1)
    send(n - 2)
    loop(0, me // 2 + 1, lambda pair: values(n - 1, pair))
    end_values(n - 1)
    send(n - 1)
    finish_blocks(src_of, dst_of, send_sem, recv_sem, local_sem, me, n, cp_size)


def attention(n, cp_size, head_dim, q, kv, collective_id):
    part, rows = q.shape[1], q.shape[2]
    heads = part // head_dim
    vmem = pl.BlockSpec(memory_space=pltpu.VMEM)
    return pl.pallas_call(
        functools.partial(attention_kernel, n, cp_size, head_dim),
        in_specs=[vmem, vmem],
        out_specs=pl.BlockSpec(memory_space=pl.ANY),
        out_shape=jax.ShapeDtypeStruct(q.shape, BF16),
        scratch_shapes=[
            pltpu.VMEM((heads, n * rows, head_dim), BF16),
            pltpu.VMEM((heads, head_dim, n * rows), BF16),
            pltpu.VMEM((2, heads, n * rows, rows), F32),
            pltpu.VMEM((2, heads, 8, rows), F32),
            pltpu.VMEM((heads, 8, rows), F32),
            pltpu.VMEM((heads, 8, rows), F32),
            pltpu.VMEM((heads, head_dim, rows), F32),
            pltpu.VMEM(q.shape, BF16),
            pltpu.SemaphoreType.DMA((n,)),
            pltpu.SemaphoreType.DMA((n,)),
            pltpu.SemaphoreType.DMA,
        ],
        compiler_params=pltpu.CompilerParams(
            collective_id=collective_id, has_side_effects=True, vmem_limit_bytes=VMEM_LIMIT
        ),
        cost_estimate=pl.CostEstimate(
            flops=2 * n * n * rows * rows * part, bytes_accessed=8 * n * part * rows, transcendentals=n * n * rows * rows
        ),
        name="attention",
    )(q, kv)


def layer_kernel(
    n, cp_size, layer, has_next, ot_ref, cur_ref, g_mlp_ref, g_next_ref, wo_ref, wg_ref, wu_ref, wd_ref, wq_ref, *refs
):
    if has_next:
        out_ref, q_ref, mixed, ot_scr, inner, ring, ring_down, sems, in_sems, buf, send_sem, recv_sem, local_sem = refs
    else:
        out_ref, mixed, ot_scr, inner, ring, ring_down, sems, in_sems = refs
    normed = mixed
    rows, width = cur_ref.shape
    hidden = wg_ref.shape[2]
    per = width // WIDE
    n_up = hidden // COLS
    n_down = width // DOWN_COLS
    first_up = per
    first_down = per + 2 * n_up
    first_q = first_down + n_down
    total = first_q + (per if has_next else 0)
    if has_next:
        me = my_index(cp_size)
        barrier_signal(n, cp_size)

    def tile_of(i):
        return lax.rem(i + me // cp_size + 1, per)

    def start(t):
        slot = lax.rem(t, LOOKAHEAD)
        narrow = ring.at[slot, :, pl.ds(0, COLS)]

        @pl.when(t < first_up)
        def _():
            pltpu.make_async_copy(wo_ref.at[layer, :, cols(t, WIDE)], ring.at[slot], sems.at[slot]).start()

        u = t - first_up
        is_up = (t >= first_up) & (t < first_down)

        @pl.when(is_up & (lax.rem(u, 2) == 0))
        def _():
            pltpu.make_async_copy(wg_ref.at[layer, :, cols(u // 2, COLS)], narrow, sems.at[slot]).start()

        @pl.when(is_up & (lax.rem(u, 2) == 1))
        def _():
            pltpu.make_async_copy(wu_ref.at[layer, :, cols(u // 2, COLS)], narrow, sems.at[slot]).start()

        @pl.when((t >= first_down) & (t < first_q))
        def _():
            pltpu.make_async_copy(
                wd_ref.at[layer, :, cols(t - first_down, DOWN_COLS)], ring_down.at[slot], sems.at[slot]
            ).start()

        if has_next:
            @pl.when((t >= first_q) & (t < total))
            def _():
                pltpu.make_async_copy(
                    wq_ref.at[layer + 1, :, cols(tile_of(t - first_q), WIDE)], ring.at[slot], sems.at[slot]
                ).start()

    def take_wide(t):
        slot = lax.rem(t, LOOKAHEAD)
        pltpu.make_async_copy(wo_ref.at[layer, :, pl.ds(0, WIDE)], ring.at[slot], sems.at[slot]).wait()
        return ring[slot]

    def take(t):
        slot = lax.rem(t, LOOKAHEAD)
        narrow = ring.at[slot, :, pl.ds(0, COLS)]
        pltpu.make_async_copy(wg_ref.at[layer, :, pl.ds(0, COLS)], narrow, sems.at[slot]).wait()
        return narrow[...]

    ot_copy = pltpu.make_async_copy(ot_ref, ot_scr, in_sems.at[0])
    cur_copy = pltpu.make_async_copy(cur_ref, out_ref, in_sems.at[1])
    ot_copy.start()
    start(jnp.int32(0))
    cur_copy.start()
    for t in range(1, LOOKAHEAD):
        start(jnp.int32(t))
    ot_copy.wait()

    def flip(i, carry):
        mixed[:, cols(i, 256)] = ot_scr[cols(i, 256), :].T
        return carry

    lax.fori_loop(0, width // 256, flip, 0)
    cur_copy.wait()

    def out_body(t, carry):
        attn = jnp.dot(mixed[...], take_wide(t), preferred_element_type=F32).astype(BF16)
        out_ref[:, cols(t, WIDE)] = (out_ref[:, cols(t, WIDE)].astype(F32) + attn.astype(F32)).astype(BF16)
        start(t + LOOKAHEAD)
        return carry

    lax.fori_loop(0, per, out_body, 0)
    norm_into(normed, out_ref, g_mlp_ref[layer:layer + 1, :])

    def up_body(j, carry):
        t = first_up + 2 * j
        inner[:, cols(j, COLS)] = jnp.dot(normed[...], take(t), preferred_element_type=F32).astype(BF16)
        start(t + LOOKAHEAD)
        up = jnp.dot(normed[...], take(t + 1), preferred_element_type=F32).astype(BF16)
        g = inner[:, cols(j, COLS)].astype(F32)
        inner[:, cols(j, COLS)] = (jax.nn.silu(g) * up.astype(F32)).astype(BF16)
        start(t + 1 + LOOKAHEAD)
        return carry

    lax.fori_loop(0, n_up, up_body, 0)

    def down_body(j, carry):
        t = first_down + j
        slot = lax.rem(t, LOOKAHEAD)
        pltpu.make_async_copy(wd_ref.at[layer, :, pl.ds(0, DOWN_COLS)], ring_down.at[slot], sems.at[slot]).wait()
        down = jnp.dot(inner[...], ring_down[slot], preferred_element_type=F32).astype(BF16)
        sl = cols(j, DOWN_COLS)
        out_ref[:, sl] = (out_ref[:, sl].astype(F32) + down.astype(F32)).astype(BF16)
        start(t + LOOKAHEAD)
        return carry

    lax.fori_loop(0, n_down, down_body, 0)
    if has_next:
        norm_into(normed, out_ref, g_next_ref[layer + 1:layer + 2, :])
        barrier_wait(n)

        def src_of(i):
            return buf.at[i]

        def dst_of(i):
            return q_ref.at[i]

        def send(i):
            for j in range(4):
                peer = 4 * tile_of(i) + lax.rem(me + j, 4)
                send_block(src_of, dst_of, send_sem, recv_sem, local_sem, peer, me, cp_size)

        def q_body(i, carry):
            transposed_tile(normed[...], take_wide(first_q + i), src_of, 4 * tile_of(i))

            @pl.when(i > 0)
            def _():
                send(i - 1)

            return carry

        lax.fori_loop(0, per, q_body, 0)
        send(jnp.int32(per - 1))
        finish_blocks(src_of, dst_of, send_sem, recv_sem, local_sem, me, n, cp_size)


def layer_dense(n, cp_size, o_t, current, g_mlp, g_next, w_o, w_gate, w_up, w_down, w_q, layer, has_next, collective_id):
    rows, width = current.shape
    hidden = w_gate.shape[2]
    part = width // n
    vmem = pl.BlockSpec(memory_space=pltpu.VMEM)
    hbm = pl.BlockSpec(memory_space=pl.ANY)
    out_shape = [jax.ShapeDtypeStruct((rows, width), BF16)]
    out_specs = [vmem]
    scratch = [
        pltpu.VMEM((rows, width), BF16),
        pltpu.VMEM((width, rows), BF16),
        pltpu.VMEM((rows, hidden), BF16),
        pltpu.VMEM((LOOKAHEAD, width, WIDE), BF16),
        pltpu.VMEM((LOOKAHEAD, hidden, DOWN_COLS), BF16),
        pltpu.SemaphoreType.DMA((LOOKAHEAD,)),
        pltpu.SemaphoreType.DMA((2,)),
    ]
    params = dict(vmem_limit_bytes=VMEM_LIMIT)
    if has_next:
        out_shape.append(jax.ShapeDtypeStruct((n, part, rows), BF16))
        out_specs.append(hbm)
        scratch += [
            pltpu.VMEM((n, part, rows), BF16),
            pltpu.SemaphoreType.DMA((n,)),
            pltpu.SemaphoreType.DMA((n,)),
            pltpu.SemaphoreType.DMA,
        ]
        params.update(collective_id=collective_id, has_side_effects=True)
    macs = rows * width * ((2 if has_next else 1) * width + 3 * hidden)
    return pl.pallas_call(
        functools.partial(layer_kernel, n, cp_size, layer, has_next),
        in_specs=[hbm] * 2 + [vmem] * 2 + [hbm] * 5,
        out_specs=out_specs,
        out_shape=out_shape,
        scratch_shapes=scratch,
        compiler_params=pltpu.CompilerParams(**params),
        cost_estimate=pl.CostEstimate(flops=2 * macs, bytes_accessed=2 * macs // rows, transcendentals=rows * hidden),
        name="layer_dense",
    )(o_t, current, g_mlp, g_next, w_o, w_gate, w_up, w_down, w_q)


def solution(mesh):
    cp_size = mesh.shape['cp']
    n = mesh.shape['sp'] * cp_size
    row_spec = P(('dp', 'sp', 'cp'), None)

    def local(hidden, g_kv, w_k, w_v, g_attn, g_mlp, w_q, w_o, w_gate, w_up, w_down):
        rows, width = hidden.shape
        num_layers, n_heads, head_dim = w_o.shape[0], w_o.shape[1], w_o.shape[2]
        w_o = w_o.reshape(num_layers, n_heads * head_dim, width)
        kv, query = first_project(n, cp_size, hidden, g_kv, g_attn, w_k, w_v, w_q)
        current = hidden
        for layer in range(num_layers):
            o_t = attention(n, cp_size, head_dim, query, kv, 2 * layer + 1).reshape(width, rows)
            has_next = layer + 1 < num_layers
            outs = layer_dense(
                n, cp_size, o_t, current, g_mlp, g_attn,
                w_o, w_gate, w_up, w_down, w_q, layer, has_next, 2 * layer + 2,
            )
            current = outs[0]
            if has_next:
                query = outs[1]
        return current

    return jax.shard_map(local, mesh=mesh, in_specs=(row_spec,) + (P(),) * 10, out_specs=row_spec, check_vma=False)
```

```python
import functools

import jax
import jax.numpy as jnp
from jax import lax
from jax.experimental import pallas as pl
from jax.experimental.pallas import tpu as pltpu
from jax.sharding import PartitionSpec as P

F32 = jnp.float32
BF16 = jnp.bfloat16
MESH = pl.DeviceIdType.MESH
NEG_BIG = -1e30
LOOKAHEAD = 4
WIDE = 768
COLS = 512
DOWN_COLS = 256
LOG2E = 1.4426950408889634
VMEM_LIMIT = 60 * 1024 * 1024


def cols(i, size):
    return pl.ds(pl.multiple_of(i * size, size), size)


def my_index(cp_size):
    return lax.axis_index('sp') * cp_size + lax.axis_index('cp')


def device(i, cp_size):
    return {'sp': i // cp_size, 'cp': lax.rem(i, cp_size)}


def barrier_signal(n, cp_size):
    me = my_index(cp_size)
    barrier = pltpu.get_barrier_semaphore()

    def body(k, carry):
        peer = lax.rem(me + k, n)
        pl.semaphore_signal(barrier, inc=1, device_id=device(peer, cp_size), device_id_type=MESH)
        return carry

    lax.fori_loop(1, n, body, 0)


def barrier_wait(n):
    pl.semaphore_wait(pltpu.get_barrier_semaphore(), n - 1)


def remote(src, dst, send_sem, recv_sem, peer, cp_size):
    return pltpu.make_async_remote_copy(
        src_ref=src, dst_ref=dst, send_sem=send_sem, recv_sem=recv_sem, device_id=device(peer, cp_size), device_id_type=MESH
    )


def send_block(src_of, dst_of, send_sem, recv_sem, local_sem, peer, me, cp_size):
    @pl.when(peer != me)
    def _():
        remote(src_of(peer), dst_of(me), send_sem.at[peer], recv_sem.at[me], peer, cp_size).start()

    @pl.when(peer == me)
    def _():
        pltpu.make_async_copy(src_of(me), dst_of(me), local_sem).start()


def finish_blocks(src_of, dst_of, send_sem, recv_sem, local_sem, me, n, cp_size):
    pltpu.make_async_copy(src_of(me), dst_of(me), local_sem).wait()

    def body(k, carry):
        peer = lax.rem(me + k, n)
        remote(src_of(peer), dst_of(peer), send_sem.at[peer], recv_sem.at[peer], peer, cp_size).wait_send()
        remote(src_of(peer), dst_of(peer), send_sem.at[peer], recv_sem.at[peer], peer, cp_size).wait_recv()
        return carry

    lax.fori_loop(1, n, body, 0)


def norm_into(dst_ref, src_ref, gain):
    rows = src_ref.shape[0]
    gain = gain.astype(F32)

    def body(i, carry):
        sl = pl.ds(pl.multiple_of(i * 32, 32), 32)
        wide = src_ref[sl, :].astype(F32)
        inv = lax.rsqrt(jnp.mean(wide * wide, axis=-1, keepdims=True) + 1e-6)
        dst_ref[sl, :] = (wide * inv * gain).astype(BF16)
        return carry

    lax.fori_loop(0, rows // 32, body, 0)


def transposed_tile(normed, weight, buf_of, first):
    out = jnp.dot(normed, weight, preferred_element_type=F32).astype(BF16).T
    size = out.shape[0] // 4
    for j in range(4):
        buf_of(first + j)[...] = out[j * size:(j + 1) * size]


def first_kernel(
    n, cp_size, x_ref, g_kv_ref, g_q_ref, wk_ref, wv_ref, wq_ref, kv_ref, q_ref,
    normed, normed_q, ring, buf, sems, send_sem, recv_sem, local_sem,
):
    me = my_index(cp_size)
    barrier_signal(n, cp_size)
    per = x_ref.shape[1] // WIDE

    def tile_of(t):
        return lax.rem(t + me // cp_size + 1, per)

    def start(t):
        slot = lax.rem(t, LOOKAHEAD)
        for i, w_ref in enumerate((wk_ref, wv_ref)):
            @pl.when(t // per == i)
            def _(w_ref=w_ref):
                pltpu.make_async_copy(w_ref.at[:, cols(tile_of(t), WIDE)], ring.at[slot], sems.at[slot]).start()

        @pl.when(t // per == 2)
        def _():
            pltpu.make_async_copy(wq_ref.at[0, :, cols(tile_of(t), WIDE)], ring.at[slot], sems.at[slot]).start()

    def dst_of(tensor):
        def of(i):
            return q_ref.at[i] if tensor == 2 else kv_ref.at[tensor, i]

        return of

    def send(tensor, t):
        for j in range(4):
            send_block(
                lambda i: buf.at[tensor, i], dst_of(tensor), send_sem.at[tensor], recv_sem.at[tensor],
                local_sem.at[tensor], 4 * tile_of(t) + j, me, cp_size,
            )

    for t in range(LOOKAHEAD):
        start(jnp.int32(t))
    norm_into(normed, x_ref, g_kv_ref[...].reshape(1, x_ref.shape[1]))
    norm_into(normed_q, x_ref, g_q_ref[0:1, :])
    barrier_wait(n)
    for tensor in range(3):
        source = normed_q if tensor == 2 else normed

        def body(i, carry, tensor=tensor, source=source):
            t = tensor * per + i
            slot = lax.rem(t, LOOKAHEAD)
            pltpu.make_async_copy(wk_ref.at[:, pl.ds(0, WIDE)], ring.at[slot], sems.at[slot]).wait()
            transposed_tile(source[...], ring[slot], lambda g: buf.at[tensor, g], 4 * tile_of(t))

            @pl.when(i > 0)
            def _():
                send(tensor, t - 1)

            start(t + LOOKAHEAD)
            return carry

        lax.fori_loop(0, per, body, 0)
        if tensor > 0:
            send(tensor - 1, jnp.int32(tensor * per - 1))
    send(2, jnp.int32(3 * per - 1))
    for tensor in range(3):
        finish_blocks(
            lambda i, tensor=tensor: buf.at[tensor, i], dst_of(tensor), send_sem.at[tensor], recv_sem.at[tensor],
            local_sem.at[tensor], me, n, cp_size,
        )


def first_project(n, cp_size, x, g_kv, g_q, w_k, w_v, w_q):
    rows, width = x.shape
    part = width // n
    vmem = pl.BlockSpec(memory_space=pltpu.VMEM)
    hbm = pl.BlockSpec(memory_space=pl.ANY)
    return pl.pallas_call(
        functools.partial(first_kernel, n, cp_size),
        in_specs=[vmem] * 3 + [hbm] * 3,
        out_specs=[hbm] * 2,
        out_shape=[jax.ShapeDtypeStruct((2, n, part, rows), BF16), jax.ShapeDtypeStruct((n, part, rows), BF16)],
        scratch_shapes=[
            pltpu.VMEM((rows, width), BF16),
            pltpu.VMEM((rows, width), BF16),
            pltpu.VMEM((LOOKAHEAD, width, WIDE), BF16),
            pltpu.VMEM((3, n, part, rows), BF16),
            pltpu.SemaphoreType.DMA((LOOKAHEAD,)),
            pltpu.SemaphoreType.DMA((3, n)),
            pltpu.SemaphoreType.DMA((3, n)),
            pltpu.SemaphoreType.DMA((3,)),
        ],
        compiler_params=pltpu.CompilerParams(collective_id=0, has_side_effects=True, vmem_limit_bytes=VMEM_LIMIT),
        cost_estimate=pl.CostEstimate(flops=6 * rows * width * width, bytes_accessed=6 * width * width, transcendentals=0),
        name="first_project",
    )(x, g_kv, g_q, w_k, w_v, w_q)


def attention_kernel(
    n, cp_size, head_dim, q_ref, kv_ref, o_ref, k_nat, v_all, s_even, s_odd, top_even, top_odd, max_scr, sum_scr, acc_scr, buf,
    send_sem, recv_sem, local_sem,
):
    me = my_index(cp_size)
    barrier_signal(n, cp_size)
    rows = q_ref.shape[2]
    heads = q_ref.shape[1] // head_dim
    span = 2 * rows
    scale = head_dim ** -0.5 * LOG2E

    def flip(u, carry):
        for h in range(heads):
            hs = slice(h * head_dim, (h + 1) * head_dim)
            k_nat[h, cols(u, rows), :] = kv_ref[0, u, hs, :].T
            v_all[h, :, cols(u, rows)] = kv_ref[1, u, hs, :]
        return carry

    lax.fori_loop(0, n, flip, 0)

    def src_of(i):
        return buf.at[i]

    def dst_of(i):
        return o_ref.at[i]

    side = n // 2
    mine = me // side

    def block_of(k):
        near = k // side
        return ((1 - mine) * (1 - near) + mine * near) * side + lax.rem(me + k + near, side)

    s_bufs, tops = (s_even, s_odd), (top_even, top_odd)

    def scores(k, pair, masked, slot):
        t = block_of(k)
        for h in range(heads):
            q_t = q_ref[t, h * head_dim:(h + 1) * head_dim, :]
            s = jnp.dot(k_nat[h, cols(pair, span), :], q_t, preferred_element_type=F32)
            if masked:
                key = lax.broadcasted_iota(jnp.int32, s.shape, 0) + pair * span
                query = lax.broadcasted_iota(jnp.int32, s.shape, 1) + t * rows
                s = jnp.where(key <= query, s, NEG_BIG)
            s_bufs[slot][h, cols(pair, span), :] = s
            top = jnp.max(s.reshape(span // 8, 8, rows), axis=0)
            tops[slot][h] = jnp.maximum(tops[slot][h], top)

    def values(pair, slot):
        for h in range(heads):
            s = s_bufs[slot][h, cols(pair, span), :].reshape(span // 8, 8, rows)
            p = jnp.exp2(s * scale - max_scr[h][None])
            sum_scr[h] = sum_scr[h] + jnp.sum(p, axis=0)
            p = p.reshape(span, rows).astype(BF16)
            acc_scr[h] = acc_scr[h] + jnp.dot(v_all[h, :, cols(pair, span)], p, preferred_element_type=F32)

    def loop(lo, hi, fn):
        def body(pair, carry):
            fn(pair)
            return carry

        lax.fori_loop(lo, hi, body, 0)

    def clear_top(slot):
        tops[slot][...] = jnp.full(tops[slot].shape, NEG_BIG, F32)

    def begin_values(slot):
        for h in range(heads):
            top = jnp.max(tops[slot][h], axis=0, keepdims=True) * scale
            max_scr[h] = jnp.broadcast_to(top, max_scr.shape[1:])
        sum_scr[...] = jnp.zeros(sum_scr.shape, F32)
        acc_scr[...] = jnp.zeros(acc_scr.shape, F32)

    def end_values(k):
        for h in range(heads):
            total = jnp.sum(sum_scr[h], axis=0, keepdims=True)
            buf[block_of(k), h * head_dim:(h + 1) * head_dim, :] = (acc_scr[h] / total).astype(BF16)

    def send(k):
        send_block(src_of, dst_of, send_sem, recv_sem, local_sem, block_of(k), me, cp_size)

    def block(k, slot):
        last = block_of(k) // 2
        last_next = block_of(k + 1) // 2
        begin_values(slot)
        clear_top(1 - slot)
        both = jnp.minimum(last, last_next)

        def fused(pair):
            scores(k + 1, pair, False, 1 - slot)
            values(pair, slot)

        loop(0, both, fused)

        @pl.when(k > 0)
        def _():
            send(k - 1)

        loop(both, last, lambda pair: values(pair, slot))
        loop(both, last_next, lambda pair: scores(k + 1, pair, False, 1 - slot))
        scores(k + 1, last_next, True, 1 - slot)
        values(last, slot)
        end_values(k)

    first = jnp.int32(0)
    clear_top(0)
    loop(0, block_of(first) // 2, lambda pair: scores(first, pair, False, 0))
    scores(first, block_of(first) // 2, True, 0)
    barrier_wait(n)

    def two_blocks(j, carry):
        block(2 * j, 0)

        @pl.when(2 * j + 1 < n - 1)
        def _():
            block(2 * j + 1, 1)

        return carry

    lax.fori_loop(0, n // 2, two_blocks, 0)
    begin_values(1)
    send(n - 2)
    loop(0, me // 2 + 1, lambda pair: values(pair, 1))
    end_values(n - 1)
    send(n - 1)
    finish_blocks(src_of, dst_of, send_sem, recv_sem, local_sem, me, n, cp_size)


def attention(n, cp_size, head_dim, q, kv, collective_id):
    part, rows = q.shape[1], q.shape[2]
    heads = part // head_dim
    vmem = pl.BlockSpec(memory_space=pltpu.VMEM)
    return pl.pallas_call(
        functools.partial(attention_kernel, n, cp_size, head_dim),
        in_specs=[vmem, vmem],
        out_specs=pl.BlockSpec(memory_space=pl.ANY),
        out_shape=jax.ShapeDtypeStruct(q.shape, BF16),
        scratch_shapes=[
            pltpu.VMEM((heads, n * rows, head_dim), BF16),
            pltpu.VMEM((heads, head_dim, n * rows), BF16),
            pltpu.VMEM((heads, n * rows, rows), F32),
            pltpu.VMEM((heads, n * rows, rows), F32),
            pltpu.VMEM((heads, 8, rows), F32),
            pltpu.VMEM((heads, 8, rows), F32),
            pltpu.VMEM((heads, 8, rows), F32),
            pltpu.VMEM((heads, 8, rows), F32),
            pltpu.VMEM((heads, head_dim, rows), F32),
            pltpu.VMEM(q.shape, BF16),
            pltpu.SemaphoreType.DMA((n,)),
            pltpu.SemaphoreType.DMA((n,)),
            pltpu.SemaphoreType.DMA,
        ],
        compiler_params=pltpu.CompilerParams(
            collective_id=collective_id, has_side_effects=True, vmem_limit_bytes=VMEM_LIMIT
        ),
        cost_estimate=pl.CostEstimate(
            flops=2 * n * n * rows * rows * part, bytes_accessed=8 * n * part * rows, transcendentals=n * n * rows * rows
        ),
        name="attention",
    )(q, kv)


def layer_kernel(
    n, cp_size, layer, has_next, ot_ref, cur_ref, g_mlp_ref, g_next_ref, wo_ref, wg_ref, wu_ref, wd_ref, wq_ref, *refs
):
    if has_next:
        out_ref, q_ref, mixed, inner, ring, ring_down, sems, buf, send_sem, recv_sem, local_sem = refs
    else:
        out_ref, mixed, inner, ring, ring_down, sems = refs
    normed = mixed
    rows, width = cur_ref.shape
    hidden = wg_ref.shape[2]
    per = width // WIDE
    n_up = hidden // COLS
    n_down = width // DOWN_COLS
    first_up = per
    first_down = per + 2 * n_up
    first_q = first_down + n_down
    total = first_q + (per if has_next else 0)
    if has_next:
        me = my_index(cp_size)
        barrier_signal(n, cp_size)

    def tile_of(i):
        return lax.rem(i + me // cp_size + 1, per)

    def start(t):
        slot = lax.rem(t, LOOKAHEAD)
        narrow = ring.at[slot, :, pl.ds(0, COLS)]

        @pl.when(t < first_up)
        def _():
            pltpu.make_async_copy(wo_ref.at[layer, :, cols(t, WIDE)], ring.at[slot], sems.at[slot]).start()

        u = t - first_up
        is_up = (t >= first_up) & (t < first_down)

        @pl.when(is_up & (lax.rem(u, 2) == 0))
        def _():
            pltpu.make_async_copy(wg_ref.at[layer, :, cols(u // 2, COLS)], narrow, sems.at[slot]).start()

        @pl.when(is_up & (lax.rem(u, 2) == 1))
        def _():
            pltpu.make_async_copy(wu_ref.at[layer, :, cols(u // 2, COLS)], narrow, sems.at[slot]).start()

        @pl.when((t >= first_down) & (t < first_q))
        def _():
            pltpu.make_async_copy(
                wd_ref.at[layer, :, cols(t - first_down, DOWN_COLS)], ring_down.at[slot], sems.at[slot]
            ).start()

        if has_next:
            @pl.when((t >= first_q) & (t < total))
            def _():
                pltpu.make_async_copy(
                    wq_ref.at[layer + 1, :, cols(tile_of(t - first_q), WIDE)], ring.at[slot], sems.at[slot]
                ).start()

    def take_wide(t):
        slot = lax.rem(t, LOOKAHEAD)
        pltpu.make_async_copy(wo_ref.at[layer, :, pl.ds(0, WIDE)], ring.at[slot], sems.at[slot]).wait()
        return ring[slot]

    def take(t):
        slot = lax.rem(t, LOOKAHEAD)
        narrow = ring.at[slot, :, pl.ds(0, COLS)]
        pltpu.make_async_copy(wg_ref.at[layer, :, pl.ds(0, COLS)], narrow, sems.at[slot]).wait()
        return narrow[...]

    for t in range(LOOKAHEAD):
        start(jnp.int32(t))

    def flip(i, carry):
        mixed[:, cols(i, 256)] = ot_ref[cols(i, 256), :].T
        return carry

    lax.fori_loop(0, width // 256, flip, 0)

    def out_body(t, carry):
        attn = jnp.dot(mixed[...], take_wide(t), preferred_element_type=F32).astype(BF16)
        out_ref[:, cols(t, WIDE)] = (cur_ref[:, cols(t, WIDE)].astype(F32) + attn.astype(F32)).astype(BF16)
        start(t + LOOKAHEAD)
        return carry

    lax.fori_loop(0, per, out_body, 0)
    norm_into(normed, out_ref, g_mlp_ref[layer:layer + 1, :])

    def up_body(j, carry):
        t = first_up + 2 * j
        inner[:, cols(j, COLS)] = jnp.dot(normed[...], take(t), preferred_element_type=F32).astype(BF16)
        start(t + LOOKAHEAD)
        up = jnp.dot(normed[...], take(t + 1), preferred_element_type=F32).astype(BF16)
        g = inner[:, cols(j, COLS)].astype(F32)
        inner[:, cols(j, COLS)] = (jax.nn.silu(g) * up.astype(F32)).astype(BF16)
        start(t + 1 + LOOKAHEAD)
        return carry

    lax.fori_loop(0, n_up, up_body, 0)

    def down_body(j, carry):
        t = first_down + j
        slot = lax.rem(t, LOOKAHEAD)
        pltpu.make_async_copy(wd_ref.at[layer, :, pl.ds(0, DOWN_COLS)], ring_down.at[slot], sems.at[slot]).wait()
        down = jnp.dot(inner[...], ring_down[slot], preferred_element_type=F32).astype(BF16)
        sl = cols(j, DOWN_COLS)
        out_ref[:, sl] = (out_ref[:, sl].astype(F32) + down.astype(F32)).astype(BF16)
        start(t + LOOKAHEAD)
        return carry

    lax.fori_loop(0, n_down, down_body, 0)
    if has_next:
        norm_into(normed, out_ref, g_next_ref[layer + 1:layer + 2, :])
        barrier_wait(n)

        def src_of(i):
            return buf.at[i]

        def dst_of(i):
            return q_ref.at[i]

        def send(i):
            for j in range(4):
                peer = 4 * tile_of(i) + j
                send_block(src_of, dst_of, send_sem, recv_sem, local_sem, peer, me, cp_size)

        def q_body(i, carry):
            transposed_tile(normed[...], take_wide(first_q + i), src_of, 4 * tile_of(i))

            @pl.when(i > 0)
            def _():
                send(i - 1)

            return carry

        lax.fori_loop(0, per, q_body, 0)
        send(jnp.int32(per - 1))
        finish_blocks(src_of, dst_of, send_sem, recv_sem, local_sem, me, n, cp_size)


def layer_dense(n, cp_size, o_t, current, g_mlp, g_next, w_o, w_gate, w_up, w_down, w_q, layer, has_next, collective_id):
    rows, width = current.shape
    hidden = w_gate.shape[2]
    part = width // n
    vmem = pl.BlockSpec(memory_space=pltpu.VMEM)
    hbm = pl.BlockSpec(memory_space=pl.ANY)
    out_shape = [jax.ShapeDtypeStruct((rows, width), BF16)]
    out_specs = [vmem]
    scratch = [
        pltpu.VMEM((rows, width), BF16),
        pltpu.VMEM((rows, hidden), BF16),
        pltpu.VMEM((LOOKAHEAD, width, WIDE), BF16),
        pltpu.VMEM((LOOKAHEAD, hidden, DOWN_COLS), BF16),
        pltpu.SemaphoreType.DMA((LOOKAHEAD,)),
    ]
    params = dict(vmem_limit_bytes=VMEM_LIMIT)
    if has_next:
        out_shape.append(jax.ShapeDtypeStruct((n, part, rows), BF16))
        out_specs.append(hbm)
        scratch += [
            pltpu.VMEM((n, part, rows), BF16),
            pltpu.SemaphoreType.DMA((n,)),
            pltpu.SemaphoreType.DMA((n,)),
            pltpu.SemaphoreType.DMA,
        ]
        params.update(collective_id=collective_id, has_side_effects=True)
    macs = rows * width * ((2 if has_next else 1) * width + 3 * hidden)
    return pl.pallas_call(
        functools.partial(layer_kernel, n, cp_size, layer, has_next),
        in_specs=[vmem] * 4 + [hbm] * 5,
        out_specs=out_specs,
        out_shape=out_shape,
        scratch_shapes=scratch,
        compiler_params=pltpu.CompilerParams(**params),
        cost_estimate=pl.CostEstimate(flops=2 * macs, bytes_accessed=2 * macs // rows, transcendentals=rows * hidden),
        name="layer_dense",
    )(o_t, current, g_mlp, g_next, w_o, w_gate, w_up, w_down, w_q)


def solution(mesh):
    cp_size = mesh.shape['cp']
    n = mesh.shape['sp'] * cp_size
    row_spec = P(('dp', 'sp', 'cp'), None)

    def local(hidden, g_kv, w_k, w_v, g_attn, g_mlp, w_q, w_o, w_gate, w_up, w_down):
        rows, width = hidden.shape
        num_layers, n_heads, head_dim = w_o.shape[0], w_o.shape[1], w_o.shape[2]
        w_o = w_o.reshape(num_layers, n_heads * head_dim, width)
        kv, query = first_project(n, cp_size, hidden, g_kv, g_attn, w_k, w_v, w_q)
        current = hidden
        for layer in range(num_layers):
            o_t = attention(n, cp_size, head_dim, query, kv, 2 * layer + 1).reshape(width, rows)
            has_next = layer + 1 < num_layers
            outs = layer_dense(
                n, cp_size, o_t, current, g_mlp, g_attn,
                w_o, w_gate, w_up, w_down, w_q, layer, has_next, 2 * layer + 2,
            )
            current = outs[0]
            if has_next:
                query = outs[1]
        return current

    return jax.shard_map(local, mesh=mesh, in_specs=(row_spec,) + (P(),) * 10, out_specs=row_spec, check_vma=False)
```

```python
import functools

import jax
import jax.numpy as jnp
from jax import lax
from jax.experimental import pallas as pl
from jax.experimental.pallas import tpu as pltpu
from jax.sharding import PartitionSpec as P

F32 = jnp.float32
BF16 = jnp.bfloat16
MESH = pl.DeviceIdType.MESH
NEG_BIG = -1e30
LOOKAHEAD = 4
WIDE = 768
COLS = 512
DOWN_COLS = 256
LOG2E = 1.4426950408889634
VMEM_LIMIT = 60 * 1024 * 1024


def cols(i, size):
    return pl.ds(pl.multiple_of(i * size, size), size)


def my_index(cp_size):
    return lax.axis_index('sp') * cp_size + lax.axis_index('cp')


def device(i, cp_size):
    return {'sp': i // cp_size, 'cp': lax.rem(i, cp_size)}


def barrier_signal(n, cp_size):
    me = my_index(cp_size)
    barrier = pltpu.get_barrier_semaphore()

    def body(k, carry):
        peer = lax.rem(me + k, n)
        pl.semaphore_signal(barrier, inc=1, device_id=device(peer, cp_size), device_id_type=MESH)
        return carry

    lax.fori_loop(1, n, body, 0)


def barrier_wait(n):
    pl.semaphore_wait(pltpu.get_barrier_semaphore(), n - 1)


def remote(src, dst, send_sem, recv_sem, peer, cp_size):
    return pltpu.make_async_remote_copy(
        src_ref=src, dst_ref=dst, send_sem=send_sem, recv_sem=recv_sem, device_id=device(peer, cp_size), device_id_type=MESH
    )


def send_block(src_of, dst_of, send_sem, recv_sem, local_sem, peer, me, cp_size):
    @pl.when(peer != me)
    def _():
        remote(src_of(peer), dst_of(me), send_sem.at[peer], recv_sem.at[me], peer, cp_size).start()

    @pl.when(peer == me)
    def _():
        pltpu.make_async_copy(src_of(me), dst_of(me), local_sem).start()


def finish_blocks(src_of, dst_of, send_sem, recv_sem, local_sem, me, n, cp_size):
    pltpu.make_async_copy(src_of(me), dst_of(me), local_sem).wait()

    def body(k, carry):
        peer = lax.rem(me + k, n)
        remote(src_of(peer), dst_of(peer), send_sem.at[peer], recv_sem.at[peer], peer, cp_size).wait_send()
        remote(src_of(peer), dst_of(peer), send_sem.at[peer], recv_sem.at[peer], peer, cp_size).wait_recv()
        return carry

    lax.fori_loop(1, n, body, 0)


def norm_into(dst_ref, src_ref, gain):
    rows = src_ref.shape[0]
    gain = gain.astype(F32)

    def body(i, carry):
        sl = pl.ds(pl.multiple_of(i * 32, 32), 32)
        wide = src_ref[sl, :].astype(F32)
        inv = lax.rsqrt(jnp.mean(wide * wide, axis=-1, keepdims=True) + 1e-6)
        dst_ref[sl, :] = (wide * inv * gain).astype(BF16)
        return carry

    lax.fori_loop(0, rows // 32, body, 0)


def transposed_tile(normed, weight, buf_of, first):
    out = jnp.dot(normed, weight, preferred_element_type=F32).astype(BF16).T
    size = out.shape[0] // 4
    for j in range(4):
        buf_of(first + j)[...] = out[j * size:(j + 1) * size]


def first_kernel(
    n, cp_size, x_ref, g_kv_ref, g_q_ref, wk_ref, wv_ref, wq_ref, kv_ref, q_ref,
    normed, normed_q, ring, buf, sems, send_sem, recv_sem, local_sem,
):
    me = my_index(cp_size)
    barrier_signal(n, cp_size)
    per = x_ref.shape[1] // WIDE

    def tile_of(t):
        return lax.rem(t + me // cp_size + 1, per)

    def start(t):
        slot = lax.rem(t, LOOKAHEAD)
        for i, w_ref in enumerate((wk_ref, wv_ref)):
            @pl.when(t // per == i)
            def _(w_ref=w_ref):
                pltpu.make_async_copy(w_ref.at[:, cols(tile_of(t), WIDE)], ring.at[slot], sems.at[slot]).start()

        @pl.when(t // per == 2)
        def _():
            pltpu.make_async_copy(wq_ref.at[0, :, cols(tile_of(t), WIDE)], ring.at[slot], sems.at[slot]).start()

    def dst_of(tensor):
        def of(i):
            return q_ref.at[i] if tensor == 2 else kv_ref.at[tensor, i]

        return of

    def send(tensor, t):
        for j in range(4):
            send_block(
                lambda i: buf.at[tensor, i], dst_of(tensor), send_sem.at[tensor], recv_sem.at[tensor],
                local_sem.at[tensor], 4 * tile_of(t) + j, me, cp_size,
            )

    for t in range(LOOKAHEAD):
        start(jnp.int32(t))
    norm_into(normed, x_ref, g_kv_ref[...].reshape(1, x_ref.shape[1]))
    barrier_wait(n)
    for tensor in range(3):
        source = normed_q if tensor == 2 else normed
        if tensor == 2:
            norm_into(normed_q, x_ref, g_q_ref[0:1, :])

        def body(i, carry, tensor=tensor, source=source):
            t = tensor * per + i
            slot = lax.rem(t, LOOKAHEAD)
            pltpu.make_async_copy(wk_ref.at[:, pl.ds(0, WIDE)], ring.at[slot], sems.at[slot]).wait()
            transposed_tile(source[...], ring[slot], lambda g: buf.at[tensor, g], 4 * tile_of(t))

            @pl.when(i > 0)
            def _():
                send(tensor, t - 1)

            start(t + LOOKAHEAD)
            return carry

        lax.fori_loop(0, per, body, 0)
        if tensor > 0:
            send(tensor - 1, jnp.int32(tensor * per - 1))
    send(2, jnp.int32(3 * per - 1))
    for tensor in range(3):
        finish_blocks(
            lambda i, tensor=tensor: buf.at[tensor, i], dst_of(tensor), send_sem.at[tensor], recv_sem.at[tensor],
            local_sem.at[tensor], me, n, cp_size,
        )


def first_project(n, cp_size, x, g_kv, g_q, w_k, w_v, w_q):
    rows, width = x.shape
    part = width // n
    vmem = pl.BlockSpec(memory_space=pltpu.VMEM)
    hbm = pl.BlockSpec(memory_space=pl.ANY)
    return pl.pallas_call(
        functools.partial(first_kernel, n, cp_size),
        in_specs=[vmem] * 3 + [hbm] * 3,
        out_specs=[hbm] * 2,
        out_shape=[jax.ShapeDtypeStruct((2, n, part, rows), BF16), jax.ShapeDtypeStruct((n, part, rows), BF16)],
        scratch_shapes=[
            pltpu.VMEM((rows, width), BF16),
            pltpu.VMEM((rows, width), BF16),
            pltpu.VMEM((LOOKAHEAD, width, WIDE), BF16),
            pltpu.VMEM((3, n, part, rows), BF16),
            pltpu.SemaphoreType.DMA((LOOKAHEAD,)),
            pltpu.SemaphoreType.DMA((3, n)),
            pltpu.SemaphoreType.DMA((3, n)),
            pltpu.SemaphoreType.DMA((3,)),
        ],
        compiler_params=pltpu.CompilerParams(collective_id=0, has_side_effects=True, vmem_limit_bytes=VMEM_LIMIT),
        cost_estimate=pl.CostEstimate(flops=6 * rows * width * width, bytes_accessed=6 * width * width, transcendentals=0),
        name="first_project",
    )(x, g_kv, g_q, w_k, w_v, w_q)


def attention_kernel(
    n, cp_size, head_dim, q_ref, kv_ref, o_ref, k_nat, v_all, s_even, s_odd, top_even, top_odd, max_scr, sum_scr, acc_scr, buf,
    send_sem, recv_sem, local_sem,
):
    me = my_index(cp_size)
    barrier_signal(n, cp_size)
    rows = q_ref.shape[2]
    heads = q_ref.shape[1] // head_dim
    span = 2 * rows
    scale = head_dim ** -0.5 * LOG2E

    def flip(u, carry):
        for h in range(heads):
            hs = slice(h * head_dim, (h + 1) * head_dim)
            k_nat[h, cols(u, rows), :] = kv_ref[0, u, hs, :].T
            v_all[h, :, cols(u, rows)] = kv_ref[1, u, hs, :]
        return carry

    lax.fori_loop(0, n, flip, 0)

    def src_of(i):
        return buf.at[i]

    def dst_of(i):
        return o_ref.at[i]

    side = n // 2
    mine = me // side

    def block_of(k):
        near = k // side
        return ((1 - mine) * (1 - near) + mine * near) * side + lax.rem(me + k + near, side)

    s_bufs, tops = (s_even, s_odd), (top_even, top_odd)

    def scores(k, pair, masked, slot):
        t = block_of(k)
        for h in range(heads):
            q_t = q_ref[t, h * head_dim:(h + 1) * head_dim, :]
            s = jnp.dot(k_nat[h, cols(pair, span), :], q_t, preferred_element_type=F32)
            if masked:
                key = lax.broadcasted_iota(jnp.int32, s.shape, 0) + pair * span
                query = lax.broadcasted_iota(jnp.int32, s.shape, 1) + t * rows
                s = jnp.where(key <= query, s, NEG_BIG)
            s_bufs[slot][h, cols(pair, span), :] = s
            top = jnp.max(s.reshape(span // 8, 8, rows), axis=0)
            tops[slot][h] = jnp.maximum(tops[slot][h], top)

    def values(pair, slot):
        for h in range(heads):
            s = s_bufs[slot][h, cols(pair, span), :].reshape(span // 8, 8, rows)
            p = jnp.exp2(s * scale - max_scr[h][None])
            sum_scr[h] = sum_scr[h] + jnp.sum(p, axis=0)
            p = p.reshape(span, rows).astype(BF16)
            acc_scr[h] = acc_scr[h] + jnp.dot(v_all[h, :, cols(pair, span)], p, preferred_element_type=F32)

    def loop(lo, hi, fn):
        def body(pair, carry):
            fn(pair)
            return carry

        lax.fori_loop(lo, hi, body, 0)

    def clear_top(slot):
        tops[slot][...] = jnp.full(tops[slot].shape, NEG_BIG, F32)

    def begin_values(slot):
        for h in range(heads):
            top = jnp.max(tops[slot][h], axis=0, keepdims=True) * scale
            max_scr[h] = jnp.broadcast_to(top, max_scr.shape[1:])
        sum_scr[...] = jnp.zeros(sum_scr.shape, F32)
        acc_scr[...] = jnp.zeros(acc_scr.shape, F32)

    def end_values(k):
        for h in range(heads):
            total = jnp.sum(sum_scr[h], axis=0, keepdims=True)
            buf[block_of(k), h * head_dim:(h + 1) * head_dim, :] = (acc_scr[h] / total).astype(BF16)

    def send(k):
        send_block(src_of, dst_of, send_sem, recv_sem, local_sem, block_of(k), me, cp_size)

    def block(k, slot):
        last = block_of(k) // 2
        last_next = block_of(k + 1) // 2
        begin_values(slot)
        clear_top(1 - slot)
        both = jnp.minimum(last, last_next)

        def fused(pair):
            scores(k + 1, pair, False, 1 - slot)
            values(pair, slot)

        loop(0, both, fused)

        @pl.when(k > 0)
        def _():
            send(k - 1)

        loop(both, last, lambda pair: values(pair, slot))
        loop(both, last_next, lambda pair: scores(k + 1, pair, False, 1 - slot))
        scores(k + 1, last_next, True, 1 - slot)
        values(last, slot)
        end_values(k)

    first = jnp.int32(0)
    clear_top(0)
    loop(0, block_of(first) // 2, lambda pair: scores(first, pair, False, 0))
    scores(first, block_of(first) // 2, True, 0)
    barrier_wait(n)

    def two_blocks(j, carry):
        block(2 * j, 0)

        @pl.when(2 * j + 1 < n - 1)
        def _():
            block(2 * j + 1, 1)

        return carry

    lax.fori_loop(0, n // 2, two_blocks, 0)
    begin_values(1)
    send(n - 2)
    loop(0, me // 2 + 1, lambda pair: values(pair, 1))
    end_values(n - 1)
    send(n - 1)
    finish_blocks(src_of, dst_of, send_sem, recv_sem, local_sem, me, n, cp_size)


def attention(n, cp_size, head_dim, q, kv, collective_id):
    part, rows = q.shape[1], q.shape[2]
    heads = part // head_dim
    vmem = pl.BlockSpec(memory_space=pltpu.VMEM)
    return pl.pallas_call(
        functools.partial(attention_kernel, n, cp_size, head_dim),
        in_specs=[vmem, vmem],
        out_specs=pl.BlockSpec(memory_space=pl.ANY),
        out_shape=jax.ShapeDtypeStruct(q.shape, BF16),
        scratch_shapes=[
            pltpu.VMEM((heads, n * rows, head_dim), BF16),
            pltpu.VMEM((heads, head_dim, n * rows), BF16),
            pltpu.VMEM((heads, n * rows, rows), F32),
            pltpu.VMEM((heads, n * rows, rows), F32),
            pltpu.VMEM((heads, 8, rows), F32),
            pltpu.VMEM((heads, 8, rows), F32),
            pltpu.VMEM((heads, 8, rows), F32),
            pltpu.VMEM((heads, 8, rows), F32),
            pltpu.VMEM((heads, head_dim, rows), F32),
            pltpu.VMEM(q.shape, BF16),
            pltpu.SemaphoreType.DMA((n,)),
            pltpu.SemaphoreType.DMA((n,)),
            pltpu.SemaphoreType.DMA,
        ],
        compiler_params=pltpu.CompilerParams(
            collective_id=collective_id, has_side_effects=True, vmem_limit_bytes=VMEM_LIMIT
        ),
        cost_estimate=pl.CostEstimate(
            flops=2 * n * n * rows * rows * part, bytes_accessed=8 * n * part * rows, transcendentals=n * n * rows * rows
        ),
        name="attention",
    )(q, kv)


def layer_kernel(
    n, cp_size, layer, has_next, ot_ref, cur_ref, g_mlp_ref, g_next_ref, wo_ref, wg_ref, wu_ref, wd_ref, wq_ref, *refs
):
    if has_next:
        out_ref, q_ref, mixed, inner, ring, ring_down, sems, buf, send_sem, recv_sem, local_sem = refs
    else:
        out_ref, mixed, inner, ring, ring_down, sems = refs
    normed = mixed
    rows, width = cur_ref.shape
    hidden = wg_ref.shape[2]
    per = width // WIDE
    n_up = hidden // COLS
    n_down = width // DOWN_COLS
    first_up = per
    first_down = per + 2 * n_up
    first_q = first_down + n_down
    total = first_q + (per if has_next else 0)
    if has_next:
        me = my_index(cp_size)
        barrier_signal(n, cp_size)

    def tile_of(i):
        return lax.rem(i + me // cp_size + 1, per)

    def start(t):
        slot = lax.rem(t, LOOKAHEAD)
        narrow = ring.at[slot, :, pl.ds(0, COLS)]

        @pl.when(t < first_up)
        def _():
            pltpu.make_async_copy(wo_ref.at[layer, :, cols(t, WIDE)], ring.at[slot], sems.at[slot]).start()

        u = t - first_up
        is_up = (t >= first_up) & (t < first_down)

        @pl.when(is_up & (lax.rem(u, 2) == 0))
        def _():
            pltpu.make_async_copy(wg_ref.at[layer, :, cols(u // 2, COLS)], narrow, sems.at[slot]).start()

        @pl.when(is_up & (lax.rem(u, 2) == 1))
        def _():
            pltpu.make_async_copy(wu_ref.at[layer, :, cols(u // 2, COLS)], narrow, sems.at[slot]).start()

        @pl.when((t >= first_down) & (t < first_q))
        def _():
            pltpu.make_async_copy(
                wd_ref.at[layer, :, cols(t - first_down, DOWN_COLS)], ring_down.at[slot], sems.at[slot]
            ).start()

        if has_next:
            @pl.when((t >= first_q) & (t < total))
            def _():
                pltpu.make_async_copy(
                    wq_ref.at[layer + 1, :, cols(tile_of(t - first_q), WIDE)], ring.at[slot], sems.at[slot]
                ).start()

    def take_wide(t):
        slot = lax.rem(t, LOOKAHEAD)
        pltpu.make_async_copy(wo_ref.at[layer, :, pl.ds(0, WIDE)], ring.at[slot], sems.at[slot]).wait()
        return ring[slot]

    def take(t):
        slot = lax.rem(t, LOOKAHEAD)
        narrow = ring.at[slot, :, pl.ds(0, COLS)]
        pltpu.make_async_copy(wg_ref.at[layer, :, pl.ds(0, COLS)], narrow, sems.at[slot]).wait()
        return narrow[...]

    for t in range(LOOKAHEAD):
        start(jnp.int32(t))

    def flip(i, carry):
        mixed[:, cols(i, 256)] = ot_ref[cols(i, 256), :].T
        return carry

    lax.fori_loop(0, width // 256, flip, 0)

    def out_body(t, carry):
        attn = jnp.dot(mixed[...], take_wide(t), preferred_element_type=F32).astype(BF16)
        out_ref[:, cols(t, WIDE)] = (cur_ref[:, cols(t, WIDE)].astype(F32) + attn.astype(F32)).astype(BF16)
        start(t + LOOKAHEAD)
        return carry

    lax.fori_loop(0, per, out_body, 0)
    norm_into(normed, out_ref, g_mlp_ref[layer:layer + 1, :])

    def up_body(j, carry):
        t = first_up + 2 * j
        inner[:, cols(j, COLS)] = jnp.dot(normed[...], take(t), preferred_element_type=F32).astype(BF16)
        start(t + LOOKAHEAD)
        up = jnp.dot(normed[...], take(t + 1), preferred_element_type=F32).astype(BF16)
        g = inner[:, cols(j, COLS)].astype(F32)
        inner[:, cols(j, COLS)] = (jax.nn.silu(g) * up.astype(F32)).astype(BF16)
        start(t + 1 + LOOKAHEAD)
        return carry

    lax.fori_loop(0, n_up, up_body, 0)

    def down_body(j, carry):
        t = first_down + j
        slot = lax.rem(t, LOOKAHEAD)
        pltpu.make_async_copy(wd_ref.at[layer, :, pl.ds(0, DOWN_COLS)], ring_down.at[slot], sems.at[slot]).wait()
        down = jnp.dot(inner[...], ring_down[slot], preferred_element_type=F32).astype(BF16)
        sl = cols(j, DOWN_COLS)
        out_ref[:, sl] = (out_ref[:, sl].astype(F32) + down.astype(F32)).astype(BF16)
        start(t + LOOKAHEAD)
        return carry

    lax.fori_loop(0, n_down, down_body, 0)
    if has_next:
        norm_into(normed, out_ref, g_next_ref[layer + 1:layer + 2, :])
        barrier_wait(n)

        def src_of(i):
            return buf.at[i]

        def dst_of(i):
            return q_ref.at[i]

        def send(i):
            for j in range(4):
                peer = 4 * tile_of(i) + j
                send_block(src_of, dst_of, send_sem, recv_sem, local_sem, peer, me, cp_size)

        def q_body(i, carry):
            transposed_tile(normed[...], take_wide(first_q + i), src_of, 4 * tile_of(i))

            @pl.when(i > 0)
            def _():
                send(i - 1)

            return carry

        lax.fori_loop(0, per, q_body, 0)
        send(jnp.int32(per - 1))
        finish_blocks(src_of, dst_of, send_sem, recv_sem, local_sem, me, n, cp_size)


def layer_dense(n, cp_size, o_t, current, g_mlp, g_next, w_o, w_gate, w_up, w_down, w_q, layer, has_next, collective_id):
    rows, width = current.shape
    hidden = w_gate.shape[2]
    part = width // n
    vmem = pl.BlockSpec(memory_space=pltpu.VMEM)
    hbm = pl.BlockSpec(memory_space=pl.ANY)
    out_shape = [jax.ShapeDtypeStruct((rows, width), BF16)]
    out_specs = [vmem]
    scratch = [
        pltpu.VMEM((rows, width), BF16),
        pltpu.VMEM((rows, hidden), BF16),
        pltpu.VMEM((LOOKAHEAD, width, WIDE), BF16),
        pltpu.VMEM((LOOKAHEAD, hidden, DOWN_COLS), BF16),
        pltpu.SemaphoreType.DMA((LOOKAHEAD,)),
    ]
    params = dict(vmem_limit_bytes=VMEM_LIMIT)
    if has_next:
        out_shape.append(jax.ShapeDtypeStruct((n, part, rows), BF16))
        out_specs.append(hbm)
        scratch += [
            pltpu.VMEM((n, part, rows), BF16),
            pltpu.SemaphoreType.DMA((n,)),
            pltpu.SemaphoreType.DMA((n,)),
            pltpu.SemaphoreType.DMA,
        ]
        params.update(collective_id=collective_id, has_side_effects=True)
    macs = rows * width * ((2 if has_next else 1) * width + 3 * hidden)
    return pl.pallas_call(
        functools.partial(layer_kernel, n, cp_size, layer, has_next),
        in_specs=[vmem] * 4 + [hbm] * 5,
        out_specs=out_specs,
        out_shape=out_shape,
        scratch_shapes=scratch,
        compiler_params=pltpu.CompilerParams(**params),
        cost_estimate=pl.CostEstimate(flops=2 * macs, bytes_accessed=2 * macs // rows, transcendentals=rows * hidden),
        name="layer_dense",
    )(o_t, current, g_mlp, g_next, w_o, w_gate, w_up, w_down, w_q)


def solution(mesh):
    cp_size = mesh.shape['cp']
    n = mesh.shape['sp'] * cp_size
    row_spec = P(('dp', 'sp', 'cp'), None)

    def local(hidden, g_kv, w_k, w_v, g_attn, g_mlp, w_q, w_o, w_gate, w_up, w_down):
        rows, width = hidden.shape
        num_layers, n_heads, head_dim = w_o.shape[0], w_o.shape[1], w_o.shape[2]
        w_o = w_o.reshape(num_layers, n_heads * head_dim, width)
        kv, query = first_project(n, cp_size, hidden, g_kv, g_attn, w_k, w_v, w_q)
        current = hidden
        for layer in range(num_layers):
            o_t = attention(n, cp_size, head_dim, query, kv, 2 * layer + 1).reshape(width, rows)
            has_next = layer + 1 < num_layers
            outs = layer_dense(
                n, cp_size, o_t, current, g_mlp, g_attn,
                w_o, w_gate, w_up, w_down, w_q, layer, has_next, 2 * layer + 2,
            )
            current = outs[0]
            if has_next:
                query = outs[1]
        return current

    return jax.shard_map(local, mesh=mesh, in_specs=(row_spec,) + (P(),) * 10, out_specs=row_spec, check_vma=False)
```
